32 devices in a mesh: group: 2 (over y), ctx: 4 (over z), head: 4 (over x, core).
Axes of the slice: x: 2, y: 2, z: 4, core: 2. Of those that a mesh axis runs over, the one named last changes fastest.
Arguments:
- query_nope: bfloat16 [512, 8192], P(('group', 'ctx'), 'head'), parts along dimension 0, may hold values from -6 to 6
- query_rope: bfloat16 [512, 4096], P(('group', 'ctx'), 'head'), parts along dimension 0, may hold values from -16 to 16
- kv_latent: bfloat16 [512, 512], P(('group', 'ctx'), 'head'), parts along dimension 0, may hold values from -1300 to 1300
- key_rope: bfloat16 [512, 64], P(('group', 'ctx')), parts along dimension 0, may hold values from -16 to 16
- latent_gain: float32 [512], replicated, may hold values from 0.1 to 1.9
- w_key: bfloat16 [512, 8192], P(None, 'head'), may hold values from -0.25 to 0.25
- w_value: bfloat16 [512, 8192], P(None, 'head'), may hold values from -0.25 to 0.25
- block_order: int32 [16], P('group'), parts along dimension 0, may hold values from 0 to 7, as said below
Outputs:
- attention_out: bfloat16 [512, 8192], P(('group', 'ctx'), 'head'), parts along dimension 0
The draws below stay inside these ranges and needn't reach their ends.
There are 2 independent parts, one for each index of `group`. The reference program is written for one: setup_inputs(seed, part) draws one part's arguments, and reference() takes and returns one part's arrays. A program takes and returns all parts, laid end to end along the dimension named above; an argument that names none is the same for every part. Nothing has to cross between parts.
Inputs may be any that keep to these rules, and one draw needn't show every extreme that they name: `block_order`: A permutation of 0 to 7. Entries 2 c and 2 c + 1, for each c < 4, add up to 7.
All inputs are finite; a program needn't handle non-finite values.
Results may differ from the reference program's by a relative error of at most 0.0081.
Values may be sent and summed in bfloat16 or wider, within the bound.
No kernel may reach another device: no remote copies, remote signals or barrier semaphores. Data moves between devices by JAX's collectives and lax.ppermute only.
A program may use at most 64 MiB of HBM per device.

```python
import jax
import jax.numpy as jnp
from jax import lax

LATENT = 512
ROPE = 64
NOPE = 128
VALUE_DIM = 128
HEADS = 64
TOK_DEV = 64
TOKENS = 256
BLOCK = 32


def draw_query_rope(key, part):
    values = jnp.clip(jax.random.normal(jax.random.fold_in(key, 22), (TOKENS, HEADS, ROPE), jnp.float32), -6.0, 6.0)
    return values.reshape(TOKENS, HEADS * ROPE).astype(jnp.bfloat16)


def draw_key_rope(key, part):
    values = jnp.clip(jax.random.normal(jax.random.fold_in(key, 32), (TOKENS, ROPE), jnp.float32), -6.0, 6.0)
    return values.astype(jnp.bfloat16)


def draw_kv_latent(key, part):
    row_scale = jnp.exp(jax.random.uniform(jax.random.fold_in(key, 41), (TOKENS, 1), jnp.float32, 0.0, jnp.log(10.0)))
    column_scale = jnp.exp(jax.random.uniform(jax.random.fold_in(key, 42), (1, LATENT), jnp.float32, 0.0, jnp.log(10.0)))
    column_scale = column_scale * jnp.exp(jnp.log(3.0) * jnp.arange(LATENT, dtype=jnp.float32)[None, :] / LATENT)
    noise = jnp.clip(jax.random.normal(jax.random.fold_in(key, 45), (TOKENS, LATENT), jnp.float32), -4.0, 4.0)
    return (noise * row_scale * column_scale).astype(jnp.bfloat16)


def draw_block_order(key, part):
    devices = TOKENS // TOK_DEV
    blocks = 2 * devices
    shuffled = jax.random.permutation(jax.random.fold_in(key, 51), devices).astype(jnp.int32)
    flipped = jax.random.randint(jax.random.fold_in(key, 52), (devices,), 0, 2).astype(jnp.int32)
    early = jnp.where(flipped == 1, blocks - 1 - shuffled, shuffled)
    late = blocks - 1 - early
    return jnp.stack([early, late], 1).reshape(blocks).astype(jnp.int32)


def block_scale(key, extent, shards, smallest, top_value):
    def one(axis_at, blocks):
        steps = jax.random.uniform(jax.random.fold_in(jax.random.fold_in(key, 6), axis_at), (blocks,), jnp.float32, smallest / len(shards), top_value / len(shards))
        return jnp.repeat(jnp.exp(steps), extent[axis_at] // blocks).reshape((-1,) + (1,) * (len(extent) - axis_at - 1))

    factor_of = one(*shards[0])
    for cut in shards[1:]:
        factor_of = factor_of * one(*cut)
    return factor_of


def scatter_about(rng, extent, deviation, bound, shards=(), kind=jnp.bfloat16):
    result = jax.random.normal(rng, extent, jnp.float32) * deviation
    if len(shards) > 0:
        result = block_scale(rng, extent, shards, -0.22, 0.18) * result
    return jnp.clip(result, min=-bound, max=bound).astype(kind)


def setup_inputs(seed: int = 0, part: int = 0) -> dict:
    arg_keys = jax.random.split(jax.random.key(seed), 9)
    part_splits = jax.random.split(jax.random.fold_in(arg_keys[8], part), 9)
    return {
        "query_nope": scatter_about(part_splits[0], (TOKENS, HEADS * NOPE), 1.0, 6.0, ((0, 4), (1, 4))),
        "query_rope": draw_query_rope(jax.random.fold_in(jax.random.fold_in(arg_keys[8], part), 71), part),
        "kv_latent": draw_kv_latent(jax.random.fold_in(jax.random.fold_in(arg_keys[8], part), 71), part),
        "key_rope": draw_key_rope(jax.random.fold_in(jax.random.fold_in(arg_keys[8], part), 71), part),
        "latent_gain": jnp.clip(1.0 + 0.18 * jax.random.normal(arg_keys[4], (LATENT,), jnp.float32), 0.1, 1.9),
        "w_key": scatter_about(arg_keys[5], (LATENT, HEADS * NOPE), LATENT ** -0.5, 0.25, ((1, 4),)),
        "w_value": scatter_about(arg_keys[6], (LATENT, HEADS * VALUE_DIM), LATENT ** -0.5, 0.25, ((1, 4),)),
        "block_order": draw_block_order(jax.random.fold_in(jax.random.fold_in(arg_keys[8], part), 71), part),
    }


EPSILON = 1e-06

def rope_angle(positions, width):
    half_width = width // 2
    frequency = jnp.exp(-jnp.log(10000.0) * jnp.arange(half_width, dtype=jnp.float32) / half_width)
    return positions.astype(jnp.float32)[:, None] * frequency[None, :]

def rotate_pairs(values, angle):
    half_width = values.shape[-1] // 2
    first_half = values[..., :half_width]
    second = values[..., half_width:]
    cosine = jnp.cos(angle)
    sine_part = jnp.sin(angle)
    return jnp.concatenate([first_half * cosine - second * sine_part, second * cosine + first_half * sine_part], -1)

def reference(query_nope, query_rope, kv_latent, key_rope, latent_gain, w_key, w_value, block_order):
    row_ids = jnp.arange(TOKENS, dtype=jnp.int32)
    position = (block_order[row_ids // BLOCK] * BLOCK + row_ids % BLOCK).astype(jnp.int32)
    latent = kv_latent.astype(jnp.float32)
    mean_square = lax.optimization_barrier(jnp.mean(latent * latent, axis=1, keepdims=True))
    normed = (latent * lax.rsqrt(mean_square + EPSILON) * latent_gain[None, :]).astype(jnp.bfloat16)
    key_angle = rope_angle(position, ROPE)
    key_rotated = rotate_pairs(key_rope.astype(jnp.float32), key_angle).astype(jnp.bfloat16)
    query_rotated = rotate_pairs(query_rope.astype(jnp.float32).reshape(TOKENS, HEADS, ROPE), key_angle[:, None, :]).astype(jnp.bfloat16)
    nope_heads = jnp.transpose(query_nope.reshape(TOKENS, HEADS, NOPE), (1, 0, 2))
    rope_heads = jnp.transpose(query_rotated, (1, 0, 2))
    key_heads = jnp.transpose(w_key.reshape(LATENT, HEADS, NOPE), (1, 0, 2))
    value_heads = jnp.transpose(w_value.reshape(LATENT, HEADS, VALUE_DIM), (1, 0, 2))
    visible = position[None, :] <= position[:, None]
    score_scale = 1.0 / (NOPE + ROPE) ** 0.5

    def one_head(operands):
        nope_part, rope_part, key_map, value_map = operands
        absorbed = lax.dot_general(nope_part, key_map, (((1,), (1,)), ((), ())), preferred_element_type=jnp.float32).astype(jnp.bfloat16)
        scores = jnp.dot(absorbed, normed.T, preferred_element_type=jnp.float32)
        scores = (scores + jnp.dot(rope_part, key_rotated.T, preferred_element_type=jnp.float32)) * score_scale
        scores = jnp.where(visible, scores, -jnp.inf)
        row_max = lax.optimization_barrier(jnp.max(scores, axis=1, keepdims=True))
        exps = jnp.where(visible, jnp.exp(scores - row_max), 0.0)
        row_total = lax.optimization_barrier(jnp.sum(exps, axis=1, keepdims=True))
        mixed = (jnp.dot(exps.astype(jnp.bfloat16), normed, preferred_element_type=jnp.float32) / row_total).astype(jnp.bfloat16)
        return jnp.dot(mixed, value_map, preferred_element_type=jnp.float32)
    per_head = lax.map(one_head, (nope_heads, rope_heads, key_heads, value_heads))
    return jnp.transpose(per_head, (1, 0, 2)).reshape(TOKENS, HEADS * VALUE_DIM).astype(jnp.bfloat16)
```

```python
import math

import jax
import jax.numpy as jnp
from jax import lax
from jax.sharding import PartitionSpec as P

ROPE = 64
NOPE = 128
VALUE_DIM = 128

EPSILON = 1e-06
NEGATIVE = -1e30


def rope_angle(positions, width):
    half_width = width // 2
    frequency = jnp.exp(-jnp.log(10000.0) * jnp.arange(half_width, dtype=jnp.float32) / half_width)
    return positions.astype(jnp.float32)[:, None] * frequency[None, :]


def rotate_pairs(values, angle):
    half_width = values.shape[-1] // 2
    first_half = values[..., :half_width]
    second = values[..., half_width:]
    cosine = jnp.cos(angle)
    sine_part = jnp.sin(angle)
    return jnp.concatenate(
        [first_half * cosine - second * sine_part, second * cosine + first_half * sine_part], -1
    )


def look_up(table, slots):
    slot_ids = jnp.arange(table.shape[0], dtype=jnp.int32)
    return jnp.sum(jnp.where(slots[:, None] == slot_ids[None, :], table[None, :], 0), axis=1)


def masks_of(size):
    masks = []
    while size > 1:
        size //= 2
        masks.append(size)
    return masks


def exchange(values, axis, mask, size):
    return lax.ppermute(values, axis, [(i, i ^ mask) for i in range(size)])


def gather_by_doubling(piece, phases):
    stack = piece[None]
    sources = [{}]
    for axis, mask, size in phases:
        stack = jnp.concatenate([stack, exchange(stack, axis, mask, size)], 0)
        sources = sources + [{**s, axis: s.get(axis, 0) ^ mask} for s in sources]
    return stack, sources


def make_per_device(ctx_size, head_size):
    phases = [("ctx", m, ctx_size) for m in masks_of(ctx_size)]
    phases += [("head", m, head_size) for m in masks_of(head_size)]

    def per_device(
        query_nope, query_rope, kv_latent, key_rope, latent_gain, w_key, w_value, block_order
    ):
        tokens_here, columns = kv_latent.shape
        heads_here = w_key.shape[1] // NOPE
        latent_width = w_key.shape[0]
        block_rows = tokens_here // 2
        score_scale = 1.0 / math.sqrt(NOPE + ROPE)
        ctx_here = lax.axis_index("ctx")
        head_here = lax.axis_index("head")

        share = tokens_here // head_size
        fold = columns // ROPE
        rope_rows = share // fold
        rope_share = lax.dynamic_slice_in_dim(key_rope, head_here * share, share, 0)
        rope_share = jnp.concatenate(jnp.split(rope_share, fold, 0), 1)
        piece = jnp.concatenate([kv_latent, rope_share], 0)
        stack, sources = gather_by_doubling(piece, phases)
        per_head = stack.reshape(head_size, ctx_size, tokens_here + rope_rows, columns)
        head_offsets = [sources[i * ctx_size].get("head", 0) for i in range(head_size)]
        ctx_offsets = [sources[i].get("ctx", 0) for i in range(ctx_size)]
        index_of = jnp.zeros((head_size,), jnp.int32).at[jnp.array(head_offsets)].set(
            jnp.arange(head_size, dtype=jnp.int32)
        )
        ordered = [
            lax.dynamic_index_in_dim(per_head, index_of[head_here ^ h], 0, False)
            for h in range(head_size)
        ]
        latent = jnp.concatenate([o[:, :tokens_here] for o in ordered], 2)
        latent = latent.reshape(ctx_size * tokens_here, latent_width).astype(jnp.float32)
        square = jnp.mean(latent * latent, axis=1, keepdims=True)
        key_latent = (latent * lax.rsqrt(square + EPSILON) * latent_gain[None, :]).astype(
            jnp.bfloat16
        )
        rope = jnp.stack(
            [
                o[:, tokens_here:, f * ROPE : (f + 1) * ROPE]
                for o in ordered
                for f in range(fold)
            ],
            1,
        ).reshape(ctx_size * tokens_here, ROPE)

        source_ctx = jnp.array(ctx_offsets, jnp.int32) ^ ctx_here
        key_slots = jnp.stack([2 * source_ctx, 2 * source_ctx + 1], 1).reshape(-1)
        lanes = jnp.arange(block_rows, dtype=jnp.int32)
        key_place = (look_up(block_order, key_slots)[:, None] * block_rows + lanes).reshape(-1)
        query_slots = 2 * ctx_here + jnp.arange(2, dtype=jnp.int32)
        query_place = (look_up(block_order, query_slots)[:, None] * block_rows + lanes).reshape(-1)
        key_rotated = rotate_pairs(rope.astype(jnp.float32), rope_angle(key_place, ROPE)).astype(
            jnp.bfloat16
        )
        query_rotated = rotate_pairs(
            query_rope.astype(jnp.float32).reshape(tokens_here, heads_here, ROPE),
            rope_angle(query_place, ROPE)[:, None, :],
        ).astype(jnp.bfloat16)
        absorbed = jnp.einsum(
            "thd,lhd->htl",
            query_nope.reshape(tokens_here, heads_here, NOPE),
            w_key.reshape(latent_width, heads_here, NOPE),
            preferred_element_type=jnp.float32,
        ).astype(jnp.bfloat16)
        scores = jnp.einsum("htl,sl->hts", absorbed, key_latent, preferred_element_type=jnp.float32)
        scores = scores + jnp.einsum(
            "thd,sd->hts", query_rotated, key_rotated, preferred_element_type=jnp.float32
        )
        visible = (key_place[None, :] <= query_place[:, None])[None]
        scores = jnp.where(visible, scores * score_scale, NEGATIVE)
        row_max = jnp.max(scores, axis=2, keepdims=True)
        exps = jnp.where(visible, jnp.exp(scores - row_max), 0.0)
        total = jnp.sum(exps, axis=2, keepdims=True)
        mixed = jnp.einsum(
            "hts,sl->htl",
            exps.astype(jnp.bfloat16),
            key_latent,
            preferred_element_type=jnp.float32,
        )
        mixed = (mixed / total).astype(jnp.bfloat16)
        output = jnp.einsum(
            "htl,lhe->the",
            mixed,
            w_value.reshape(latent_width, heads_here, VALUE_DIM),
            preferred_element_type=jnp.float32,
        )
        return output.astype(jnp.bfloat16).reshape(tokens_here, heads_here * VALUE_DIM)

    return per_device


def solution(mesh):
    return jax.shard_map(
        make_per_device(mesh.shape["ctx"], mesh.shape["head"]),
        mesh=mesh,
        in_specs=(
            P(("group", "ctx"), "head"),
            P(("group", "ctx"), "head"),
            P(("group", "ctx"), "head"),
            P(("group", "ctx"), None),
            P(),
            P(None, "head"),
            P(None, "head"),
            P("group"),
        ),
        out_specs=P(("group", "ctx"), "head"),
        check_vma=False,
    )
```

```python
import functools
import math

import jax
import jax.numpy as jnp
from jax import lax
from jax.experimental import pallas as pl
from jax.experimental.pallas import tpu as pltpu
from jax.sharding import PartitionSpec as P

ROPE = 64
NOPE = 128
VALUE_DIM = 128
LANES = 128

EPSILON = 1e-06
NEGATIVE = -1e30
SCALE = math.log2(math.e) / math.sqrt(NOPE + ROPE)


BF16 = jnp.bfloat16
F32 = jnp.float32
VMEM = pl.BlockSpec(memory_space=pltpu.VMEM)
SMEM = pl.BlockSpec(memory_space=pltpu.SMEM)
ANY = pl.BlockSpec(memory_space=pl.ANY)


def masks_of(size):
    masks = []
    while size > 1:
        size //= 2
        masks.append(size)
    return masks


def gather_by_doubling(piece, phases):
    stack = piece[None]
    for axis, mask, size in phases:
        pairs = [(i, i ^ mask) for i in range(size)]
        stack = jnp.concatenate([stack, lax.ppermute(stack, axis, pairs)], 0)
    return stack


def spread_bits(index, masks):
    offset = 0
    for bit, mask in enumerate(masks):
        offset = offset + ((index >> bit) & 1) * mask
    return offset


def swap_halves(values):
    half = ROPE // 2
    lane = lax.broadcasted_iota(jnp.int32, values.shape, 1)
    width = values.shape[1]
    return jnp.where(
        lane % ROPE < half, pltpu.roll(values, width - half, 1), pltpu.roll(values, half, 1)
    )


def rotation_tables(place):
    half = ROPE // 2
    lane = lax.broadcasted_iota(jnp.int32, place.shape, 1)
    frequency = jnp.exp(-math.log(10000.0) * (lane % half).astype(F32) / half)
    angle = place.astype(F32) * frequency
    sine = jnp.sin(angle)
    return jnp.cos(angle), jnp.where(lane % ROPE < half, -sine, sine)


def places_of(token, early, late, block_rows):
    return jnp.where(token < block_rows, early, late) * block_rows + token % block_rows


def pack_kernel(latent_ref, rope_ref, piece_ref, *, share):
    tokens = latent_ref.shape[0]
    fold = LANES // ROPE
    rows = share // fold
    first = lax.axis_index("head") * share
    piece_ref[:tokens] = latent_ref[...]
    mine = rope_ref[pl.ds(pl.multiple_of(first, share), share), :].astype(F32)
    parts = [mine[f * rows : (f + 1) * rows] for f in range(fold)]
    piece_ref[tokens:] = jnp.concatenate(parts, 1).astype(BF16)


def prepare_kernel(
    order_ref, nope_ref, rope_ref, w_key_ref, query_ref, *, heads
):
    tokens = nope_ref.shape[0]
    latent_width = w_key_ref.shape[0]
    block_rows = tokens // 2
    fold = LANES // ROPE
    ctx_here = lax.axis_index("ctx")
    early = order_ref[2 * ctx_here]
    late = order_ref[2 * ctx_here + 1]
    token = lax.broadcasted_iota(jnp.int32, (tokens, LANES), 0)
    lane = lax.broadcasted_iota(jnp.int32, (tokens, LANES), 1)
    cosine, sine = rotation_tables(places_of(token, early, late, block_rows))
    for pair in range(heads // fold):
        values = rope_ref[:, pair * LANES : (pair + 1) * LANES].astype(F32)
        rotated = values * cosine + swap_halves(values) * sine
        for f in range(fold):
            head = pair * fold + f
            kept = jnp.where(lane // ROPE == f, rotated, 0.0)
            query_ref[head * tokens : (head + 1) * tokens, latent_width:] = kept.astype(BF16)
    for head in range(heads):
        columns = slice(head * NOPE, (head + 1) * NOPE)
        absorbed = lax.dot_general(
            nope_ref[:, columns],
            w_key_ref[:, columns],
            (((1,), (1,)), ((), ())),
            preferred_element_type=F32,
        )
        query_ref[head * tokens : (head + 1) * tokens, :latent_width] = absorbed.astype(BF16)


def table_kernel(order_ref, cos_ref, sin_ref, *, ctx_masks, tokens, share):
    fold = LANES // ROPE
    rows = share // fold
    block_rows = tokens // 2
    ctx_count, table_rows, _ = cos_ref.shape
    ctx_here = lax.axis_index("ctx")
    row = lax.broadcasted_iota(jnp.int32, (table_rows, LANES), 0)
    lane = lax.broadcasted_iota(jnp.int32, (table_rows, LANES), 1)
    token = (row // rows) * share + (lane // ROPE) * rows + row % rows

    def one(c, unused):
        source = ctx_here ^ spread_bits(c, ctx_masks)
        place = places_of(token, order_ref[2 * source], order_ref[2 * source + 1], block_rows)
        cos_ref[c], sin_ref[c] = rotation_tables(place)
        return unused

    if ctx_count <= 8:
        for c in range(ctx_count):
            one(c, 0)
    else:
        lax.fori_loop(0, ctx_count, one, 0)


def attend_kernel(
    order_ref,
    stack_ref,
    query_ref,
    cos_ref,
    sin_ref,
    gain_ref,
    w_value_ref,
    out_ref,
    key_ref,
    *run_refs,
    ctx_masks,
    head_masks,
    share,
    group,
    chunks_per_block,
):
    tokens = out_ref.shape[0]
    columns = stack_ref.shape[2]
    latent_width = w_value_ref.shape[0]
    heads = w_value_ref.shape[1] // VALUE_DIM
    ctx_count = cos_ref.shape[0]
    head_count = latent_width // columns
    block_rows = tokens // 2
    fold = LANES // ROPE
    rope_rows = share // fold
    ctx_here = lax.axis_index("ctx")
    head_here = lax.axis_index("head")

    def slots_of(c):
        source = ctx_here ^ spread_bits(c, ctx_masks)
        return order_ref[2 * source], order_ref[2 * source + 1]

    places = [
        spread_bits(head_here ^ h, [1 << head_masks.index(1 << b) for b in range(len(head_masks))])
        for h in range(head_count)
    ]
    lane = lax.broadcasted_iota(jnp.int32, (rope_rows, LANES), 1)

    def one_chunk(c, unused):
        first = c * tokens
        if not isinstance(c, int):
            first = pl.multiple_of(first, tokens)
        rows = pl.ds(first, tokens)
        parts = [stack_ref[p * ctx_count + c, :tokens, :].astype(F32) for p in places]
        square = functools.reduce(jnp.add, [x * x for x in parts])
        mean = jnp.sum(square, axis=1, keepdims=True) * (1.0 / latent_width)
        factor = lax.rsqrt(mean + EPSILON)
        for h, x in enumerate(parts):
            gain = gain_ref[:, h * columns : (h + 1) * columns]
            key_ref[rows, h * columns : (h + 1) * columns] = (x * factor * gain).astype(BF16)
        pieces = []
        for h, p in enumerate(places):
            values = stack_ref[p * ctx_count + c, tokens:, :].astype(F32)
            table = slice(h * rope_rows, (h + 1) * rope_rows)
            values = values * cos_ref[c, table] + swap_halves(values) * sin_ref[c, table]
            turned = pltpu.roll(values, ROPE, 1)
            pieces.append(jnp.where(lane < ROPE, values, turned))
            pieces.append(jnp.where(lane < ROPE, turned, values))
        key_ref[rows, latent_width:] = jnp.concatenate(pieces, 0).astype(BF16)
        return unused

    if ctx_count <= 8:
        for c in range(ctx_count):
            one_chunk(c, 0)
    else:
        lax.fori_loop(0, ctx_count, one_chunk, 0)

    block = chunks_per_block * tokens
    block_count = ctx_count // chunks_per_block
    query_token = lax.broadcasted_iota(jnp.int32, (tokens, block), 0)
    query_place = places_of(
        query_token, order_ref[2 * ctx_here], order_ref[2 * ctx_here + 1], block_rows
    )
    key_lane = lax.broadcasted_iota(jnp.int32, (tokens, block), 1)

    def bias_of(b):
        key_place = None
        for i in range(chunks_per_block):
            early, late = slots_of(b * chunks_per_block + i)
            place = places_of(key_lane % tokens, early, late, block_rows)
            key_place = place if i == 0 else jnp.where(key_lane < i * tokens, key_place, place)
        return jnp.where(key_place <= query_place, 0.0, NEGATIVE)

    def scores_of(query, keys, bias):
        scores = lax.dot_general(
            query, keys, (((1,), (1,)), ((), ())), preferred_element_type=F32
        )
        return scores.reshape(group, tokens, block) * SCALE + bias[None]

    def finish(g, mixed, total):
        mixed = (mixed * (1.0 / total)).astype(BF16)
        for i in range(group):
            head = g * group + i
            where = slice(head * VALUE_DIM, (head + 1) * VALUE_DIM)
            out_ref[:, where] = jnp.dot(
                mixed[i * tokens : (i + 1) * tokens],
                w_value_ref[:, where],
                preferred_element_type=F32,
            ).astype(BF16)

    if block_count == 1:
        bias = bias_of(0)
        for g in range(heads // group):
            query = query_ref[g * group * tokens : (g + 1) * group * tokens, :]
            scores = scores_of(query, key_ref[...], bias)
            exps = jnp.exp2(scores - jnp.max(scores, axis=2, keepdims=True))
            total = jnp.sum(exps, axis=2, keepdims=True).reshape(group * tokens, 1)
            mixed = jnp.dot(
                exps.reshape(group * tokens, block).astype(BF16),
                key_ref[:, :latent_width],
                preferred_element_type=F32,
            )
            finish(g, mixed, total)
        return

    max_ref, total_ref, mixed_ref = run_refs
    for g in range(heads // group):
        max_ref[...] = jnp.full(max_ref.shape, NEGATIVE, F32)
        total_ref[...] = jnp.zeros(total_ref.shape, F32)
        mixed_ref[...] = jnp.zeros(mixed_ref.shape, F32)
        query = query_ref[g * group * tokens : (g + 1) * group * tokens, :]

        def one_block(b, unused):
            keys = key_ref[pl.ds(pl.multiple_of(b * block, block), block), :]
            bias = bias_of(b)
            scores = scores_of(query, keys, bias)
            old = max_ref[:, :1].reshape(group, tokens, 1)
            new = jnp.maximum(old, jnp.max(scores, axis=2, keepdims=True))
            exps = jnp.where(bias[None] < 0.0, 0.0, jnp.exp2(scores - new))
            shrink = jnp.exp2(old - new).reshape(group * tokens, 1)
            total = jnp.sum(exps, axis=2, keepdims=True).reshape(group * tokens, 1)
            max_ref[...] = jnp.broadcast_to(new.reshape(group * tokens, 1), max_ref.shape)
            total_ref[...] = total_ref[...] * shrink + total
            mixed_ref[...] = mixed_ref[...] * shrink + jnp.dot(
                exps.reshape(group * tokens, block).astype(BF16),
                keys[:, :latent_width],
                preferred_element_type=F32,
            )
            return unused

        lax.fori_loop(0, block_count, one_block, 0)
        finish(g, mixed_ref[...], total_ref[:, :1])


def make_per_device(ctx_size, head_size):
    ctx_masks = masks_of(ctx_size)
    head_masks = masks_of(head_size)
    phases = [("ctx", m, ctx_size) for m in ctx_masks]
    phases += [("head", m, head_size) for m in head_masks]

    def per_device(
        query_nope, query_rope, kv_latent, key_rope, latent_gain, w_key, w_value, block_order
    ):
        tokens, columns = kv_latent.shape
        heads = w_key.shape[1] // NOPE
        latent_width = w_key.shape[0]
        share = tokens // head_size
        rope_rows = share * ROPE // LANES
        group = min(4, heads)
        chunks_per_block = min(ctx_size, max(1, 256 // tokens))

        piece = pl.pallas_call(
            functools.partial(pack_kernel, share=share),
            out_shape=jax.ShapeDtypeStruct((tokens + rope_rows, columns), BF16),
            in_specs=[VMEM, VMEM],
            out_specs=VMEM,
            name="pack",
        )(kv_latent, key_rope)
        stack = gather_by_doubling(piece, phases)

        query = pl.pallas_call(
            functools.partial(prepare_kernel, heads=heads),
            out_shape=jax.ShapeDtypeStruct((heads * tokens, latent_width + LANES), BF16),
            in_specs=[SMEM, VMEM, VMEM, VMEM],
            out_specs=VMEM,
            name="prepare",
        )(block_order, query_nope, query_rope, w_key)
        table = jax.ShapeDtypeStruct((ctx_size, head_size * rope_rows, LANES), F32)
        cosine, sine = pl.pallas_call(
            functools.partial(table_kernel, ctx_masks=ctx_masks, tokens=tokens, share=share),
            out_shape=(table, table),
            in_specs=[SMEM],
            out_specs=(VMEM, VMEM),
            name="tables",
        )(block_order)

        keys = ctx_size * tokens
        scratch = [pltpu.VMEM((keys, latent_width + LANES), BF16)]
        if ctx_size > chunks_per_block:
            scratch += [
                pltpu.VMEM((group * tokens, LANES), F32),
                pltpu.VMEM((group * tokens, LANES), F32),
                pltpu.VMEM((group * tokens, latent_width), F32),
            ]
        return pl.pallas_call(
            functools.partial(
                attend_kernel,
                ctx_masks=ctx_masks,
                head_masks=head_masks,
                share=share,
                group=group,
                chunks_per_block=chunks_per_block,
            ),
            out_shape=jax.ShapeDtypeStruct((tokens, heads * VALUE_DIM), BF16),
            in_specs=[SMEM, VMEM, VMEM, VMEM, VMEM, VMEM, VMEM],
            out_specs=VMEM,
            scratch_shapes=scratch,
            name="attend",
        )(
            block_order,
            stack,
            query,
            cosine,
            sine,
            latent_gain.reshape(1, latent_width),
            w_value,
        )

    return per_device


def solution(mesh):
    return jax.shard_map(
        make_per_device(mesh.shape["ctx"], mesh.shape["head"]),
        mesh=mesh,
        in_specs=(
            P(("group", "ctx"), "head"),
            P(("group", "ctx"), "head"),
            P(("group", "ctx"), "head"),
            P(("group", "ctx"), None),
            P(),
            P(None, "head"),
            P(None, "head"),
            P("group"),
        ),
        out_specs=P(("group", "ctx"), "head"),
        check_vma=False,
    )
```

```python
import functools
import math

import jax
import jax.numpy as jnp
from jax import lax
from jax.experimental import pallas as pl
from jax.experimental.pallas import tpu as pltpu
from jax.sharding import PartitionSpec as P

ROPE = 64
NOPE = 128
VALUE_DIM = 128
LANES = 128

EPSILON = 1e-06
NEGATIVE = -1e30
SCALE = math.log2(math.e) / math.sqrt(NOPE + ROPE)


BF16 = jnp.bfloat16
F32 = jnp.float32
VMEM = pl.BlockSpec(memory_space=pltpu.VMEM)
ANY = pl.BlockSpec(memory_space=pl.ANY)
HBM = pl.BlockSpec(memory_space=pltpu.MemorySpace.HBM)
MIB = 1 << 20


def masks_of(size):
    masks = []
    while size > 1:
        size //= 2
        masks.append(size)
    return masks


def spread_bits(index, masks):
    offset = 0
    for bit, mask in enumerate(masks):
        offset = offset + ((index >> bit) & 1) * mask
    return offset


def swap_halves(values):
    half = ROPE // 2
    lane = lax.broadcasted_iota(jnp.int32, values.shape, 1)
    width = values.shape[1]
    return jnp.where(
        lane % ROPE < half, pltpu.roll(values, width - half, 1), pltpu.roll(values, half, 1)
    )


def rotation_tables(place):
    half = ROPE // 2
    lane = lax.broadcasted_iota(jnp.int32, place.shape, 1)
    frequency = jnp.exp(-math.log(10000.0) * (lane % half).astype(F32) / half)
    angle = place.astype(F32) * frequency
    sine = jnp.sin(angle)
    return jnp.cos(angle), jnp.where(lane % ROPE < half, -sine, sine)


def places_of(token, early, late, block_rows):
    return jnp.where(token < block_rows, early, late) * block_rows + token % block_rows


def pack_kernel(latent_hbm, rope_hbm, piece_ref, rope_ref, sems, *, share):
    tokens = latent_hbm.shape[0]
    fold = LANES // ROPE
    rows = share // fold
    first = pl.multiple_of(lax.axis_index("head") * share, share)
    latent_copy = pltpu.make_async_copy(latent_hbm, piece_ref.at[pl.ds(0, tokens)], sems.at[0])
    rope_copy = pltpu.make_async_copy(rope_hbm.at[pl.ds(first, share)], rope_ref, sems.at[1])
    latent_copy.start()
    rope_copy.start()
    rope_copy.wait()
    mine = rope_ref[...].astype(F32)
    parts = [mine[f * rows : (f + 1) * rows] for f in range(fold)]
    piece_ref[tokens:] = jnp.concatenate(parts, 1).astype(BF16)
    latent_copy.wait()


def absorb_kernel(
    *refs, first_head, heads, with_tables
):
    if with_tables:
        (_, order_hbm, nope_hbm, rope_hbm, w_key_hbm, query_ref, cos_ref, sin_ref) = refs[:8]
        order_ref, nope_ref, rope_ref, w_key_ref, sems = refs[8:]
    else:
        (_, cos_ref, sin_ref, nope_hbm, rope_hbm, w_key_hbm, query_ref) = refs[:7]
        nope_ref, rope_ref, w_key_ref, sems = refs[7:]
    tokens = nope_hbm.shape[0]
    latent_width = w_key_hbm.shape[0]
    block_rows = tokens // 2
    fold = LANES // ROPE
    chunk = 2 * NOPE
    chunks = heads * NOPE // chunk
    copies = []
    if with_tables:
        order_copy = pltpu.make_async_copy(order_hbm, order_ref, sems.at[chunks + 2])
        order_copy.start()
    nope_copy = pltpu.make_async_copy(
        nope_hbm.at[:, pl.ds(first_head * NOPE, heads * NOPE)], nope_ref, sems.at[chunks]
    )
    nope_copy.start()
    for i in range(chunks):
        where = pl.ds(i * chunk, chunk)
        source = pl.ds(first_head * NOPE + i * chunk, chunk)
        copies.append(
            pltpu.make_async_copy(w_key_hbm.at[:, source], w_key_ref.at[:, where], sems.at[i])
        )
        copies[-1].start()
    rope_copy = pltpu.make_async_copy(
        rope_hbm.at[:, pl.ds(first_head * ROPE, heads * ROPE)], rope_ref, sems.at[chunks + 1]
    )
    rope_copy.start()
    if with_tables:
        order_copy.wait()
        ctx_here = lax.axis_index("ctx")
        early = order_ref[2 * ctx_here]
        late = order_ref[2 * ctx_here + 1]
        token = lax.broadcasted_iota(jnp.int32, (tokens, LANES), 0)
        cos_ref[...], sin_ref[...] = rotation_tables(places_of(token, early, late, block_rows))
    nope_copy.wait()
    for i in range(chunks):
        copies[i].wait()
        for head in range(i * chunk // NOPE, (i + 1) * chunk // NOPE):
            columns = slice(head * NOPE, (head + 1) * NOPE)
            absorbed = lax.dot_general(
                nope_ref[:, columns],
                w_key_ref[:, columns],
                (((1,), (1,)), ((), ())),
                preferred_element_type=F32,
            )
            query_ref[head * tokens : (head + 1) * tokens, :latent_width] = absorbed.astype(BF16)
    rope_copy.wait()
    lane = lax.broadcasted_iota(jnp.int32, (tokens, LANES), 1)
    for pair in range(heads // fold):
        values = rope_ref[:, pair * LANES : (pair + 1) * LANES].astype(F32)
        rotated = values * cos_ref[...] + swap_halves(values) * sin_ref[...]
        for f in range(fold):
            head = pair * fold + f
            kept = jnp.where(lane // ROPE == f, rotated, 0.0)
            query_ref[head * tokens : (head + 1) * tokens, latent_width:] = kept.astype(BF16)


def table_kernel(
    _, order_hbm, cos_ref, sin_ref, bias_ref, order_ref, sem, *, ctx_masks, tokens, share
):
    fold = LANES // ROPE
    rows = share // fold
    block_rows = tokens // 2
    ctx_count, table_rows, _ = cos_ref.shape
    order_copy = pltpu.make_async_copy(order_hbm, order_ref, sem.at[0])
    order_copy.start()
    order_copy.wait()
    ctx_here = lax.axis_index("ctx")
    row = lax.broadcasted_iota(jnp.int32, (table_rows, LANES), 0)
    lane = lax.broadcasted_iota(jnp.int32, (table_rows, LANES), 1)
    token = (row // rows) * share + (lane // ROPE) * rows + row % rows
    blocks, _, block = bias_ref.shape
    chunks_per_block = block // tokens
    query_token = lax.broadcasted_iota(jnp.int32, (tokens, block), 0)
    query_place = places_of(
        query_token, order_ref[2 * ctx_here], order_ref[2 * ctx_here + 1], block_rows
    )
    key_lane = lax.broadcasted_iota(jnp.int32, (tokens, block), 1)

    def one(b, unused):
        key_place = None
        for i in range(chunks_per_block):
            c = b * chunks_per_block + i
            source = ctx_here ^ spread_bits(c, ctx_masks)
            early = order_ref[2 * source]
            late = order_ref[2 * source + 1]
            cos_ref[c], sin_ref[c] = rotation_tables(places_of(token, early, late, block_rows))
            place = places_of(key_lane % tokens, early, late, block_rows)
            key_place = place if i == 0 else jnp.where(key_lane < i * tokens, key_place, place)
        bias_ref[b] = jnp.where(key_place <= query_place, 0.0, NEGATIVE)
        return unused

    if blocks == 1:
        one(0, 0)
    else:
        lax.fori_loop(0, blocks, one, 0)


def attend_kernel(
    stack_ref,
    first_ref,
    second_ref,
    cos_ref,
    sin_ref,
    bias_ref,
    gain_ref,
    w_value_ref,
    out_hbm,
    key_ref,
    out_ref,
    sems,
    *run_refs,
    head_masks,
    share,
    group,
):
    tokens = bias_ref.shape[1]
    columns = stack_ref.shape[2]
    latent_width = w_value_ref.shape[0]
    heads = w_value_ref.shape[1] // VALUE_DIM
    ctx_count = cos_ref.shape[0]
    head_count = latent_width // columns
    fold = LANES // ROPE
    rope_rows = share // fold
    groups = heads // group
    height = group * tokens
    head_here = lax.axis_index("head")
    bit_places = [1 << head_masks.index(1 << b) for b in range(len(head_masks))]
    places = [spread_bits(head_here ^ h, bit_places) for h in range(head_count)]
    lane = lax.broadcasted_iota(jnp.int32, (rope_rows, LANES), 1)

    def one_chunk(c, unused):
        first = c * tokens
        if not isinstance(c, int):
            first = pl.multiple_of(first, tokens)
        rows = pl.ds(first, tokens)
        parts = [stack_ref[p * ctx_count + c, :tokens, :].astype(F32) for p in places]
        square = functools.reduce(jnp.add, [x * x for x in parts])
        mean = jnp.sum(square, axis=1, keepdims=True) * (1.0 / latent_width)
        factor = lax.rsqrt(mean + EPSILON)
        for h, x in enumerate(parts):
            gain = gain_ref[:, h * columns : (h + 1) * columns]
            key_ref[rows, h * columns : (h + 1) * columns] = (x * factor * gain).astype(BF16)
        pieces = []
        for h, p in enumerate(places):
            values = stack_ref[p * ctx_count + c, tokens:, :].astype(F32)
            table = slice(h * rope_rows, (h + 1) * rope_rows)
            values = values * cos_ref[c, table] + swap_halves(values) * sin_ref[c, table]
            turned = pltpu.roll(values, ROPE, 1)
            pieces.append(jnp.where(lane < ROPE, values, turned))
            pieces.append(jnp.where(lane < ROPE, turned, values))
        key_ref[rows, latent_width:] = jnp.concatenate(pieces, 0).astype(BF16)
        return unused

    if ctx_count <= 8:
        for c in range(ctx_count):
            one_chunk(c, 0)
    else:
        lax.fori_loop(0, ctx_count, one_chunk, 0)

    def query_of(g):
        half = groups // 2
        ref = first_ref if g < half else second_ref
        return ref[(g % half) * height : (g % half + 1) * height, :]

    def scores_of(query, keys):
        return lax.dot_general(query, keys, (((1,), (1,)), ((), ())), preferred_element_type=F32)

    def masked(scores, b):
        return scores.reshape(group, tokens, -1) * SCALE + bias_ref[b][None]

    def out_copy(g):
        where = pl.ds(g * group * VALUE_DIM, group * VALUE_DIM)
        return pltpu.make_async_copy(out_ref.at[:, where], out_hbm.at[:, where], sems.at[g])

    def finish(g, mixed, total):
        mixed = (mixed * (1.0 / total)).astype(BF16)
        for i in range(group):
            head = g * group + i
            where = slice(head * VALUE_DIM, (head + 1) * VALUE_DIM)
            out_ref[:, where] = jnp.dot(
                mixed[i * tokens : (i + 1) * tokens],
                w_value_ref[:, where],
                preferred_element_type=F32,
            ).astype(BF16)
        out_copy(g).start()

    if bias_ref.shape[0] == 1:
        scores = scores_of(query_of(0), key_ref[...])
        for g in range(groups):
            now = masked(scores, 0)
            if g + 1 < groups:
                scores = scores_of(query_of(g + 1), key_ref[...])
            exps = jnp.exp2(now - jnp.max(now, axis=2, keepdims=True))
            total = jnp.sum(exps, axis=2, keepdims=True).reshape(height, 1)
            mixed = jnp.dot(
                exps.reshape(height, -1).astype(BF16),
                key_ref[:, :latent_width],
                preferred_element_type=F32,
            )
            finish(g, mixed, total)
    else:
        max_ref, total_ref, mixed_ref = run_refs
        block = bias_ref.shape[2]
        for g in range(groups):
            max_ref[...] = jnp.full(max_ref.shape, NEGATIVE, F32)
            total_ref[...] = jnp.zeros(total_ref.shape, F32)
            mixed_ref[...] = jnp.zeros(mixed_ref.shape, F32)
            query = query_of(g)

            def one_block(b, unused):
                keys = key_ref[pl.ds(pl.multiple_of(b * block, block), block), :]
                now = masked(scores_of(query, keys), b)
                old = max_ref[:, :1].reshape(group, tokens, 1)
                new = jnp.maximum(old, jnp.max(now, axis=2, keepdims=True))
                exps = jnp.where(bias_ref[b][None] < 0.0, 0.0, jnp.exp2(now - new))
                shrink = jnp.exp2(old - new).reshape(height, 1)
                total = jnp.sum(exps, axis=2, keepdims=True).reshape(height, 1)
                max_ref[...] = jnp.broadcast_to(new.reshape(height, 1), max_ref.shape)
                total_ref[...] = total_ref[...] * shrink + total
                mixed_ref[...] = mixed_ref[...] * shrink + jnp.dot(
                    exps.reshape(height, block).astype(BF16),
                    keys[:, :latent_width],
                    preferred_element_type=F32,
                )
                return unused

            lax.fori_loop(0, bias_ref.shape[0], one_block, 0)
            finish(g, mixed_ref[...], total_ref[:, :1])
    for g in range(groups):
        out_copy(g).wait()


def make_per_device(ctx_size, head_size):
    ctx_masks = masks_of(ctx_size)
    head_masks = masks_of(head_size)

    def per_device(
        query_nope, query_rope, kv_latent, key_rope, latent_gain, w_key, w_value, block_order
    ):
        tokens, columns = kv_latent.shape
        heads = w_key.shape[1] // NOPE
        latent_width = w_key.shape[0]
        query_nope, query_rope, kv_latent, key_rope, w_key, block_order = (
            pltpu.with_memory_space_constraint(x, pltpu.MemorySpace.HBM)
            for x in (query_nope, query_rope, kv_latent, key_rope, w_key, block_order)
        )
        share = tokens // head_size
        rope_rows = share * ROPE // LANES
        group = min(4, heads // 2)
        half = heads // 2
        chunks_per_block = min(ctx_size, max(1, 256 // tokens))
        blocks = ctx_size // chunks_per_block

        def double(stack, axis, mask, size):
            pairs = [(i, i ^ mask) for i in range(size)]
            return jnp.concatenate([stack, lax.ppermute(stack, axis, pairs)], 0)

        def absorb(after, first_head, tables):
            rope_table = jax.ShapeDtypeStruct((tokens, LANES), F32)
            query = jax.ShapeDtypeStruct((half * tokens, latent_width + LANES), BF16)
            with_tables = tables is None
            chunks = half // 2
            scratch = [pltpu.SMEM(block_order.shape, jnp.int32)] if with_tables else []
            return pl.pallas_call(
                functools.partial(
                    absorb_kernel, first_head=first_head, heads=half, with_tables=with_tables
                ),
                out_shape=(query, rope_table, rope_table) if with_tables else query,
                in_specs=[ANY, HBM, HBM, HBM, HBM]
                if with_tables
                else [ANY, VMEM, VMEM, HBM, HBM, HBM],
                out_specs=(VMEM, VMEM, VMEM) if with_tables else VMEM,
                scratch_shapes=scratch
                + [
                    pltpu.VMEM((tokens, half * NOPE), BF16),
                    pltpu.VMEM((tokens, half * ROPE), BF16),
                    pltpu.VMEM((latent_width, half * NOPE), BF16),
                    pltpu.SemaphoreType.DMA((chunks + 3,)),
                ],
                compiler_params=pltpu.CompilerParams(vmem_limit_bytes=6 * MIB),
                name="absorb",
            )(
                after,
                *((block_order,) if with_tables else tables),
                query_nope,
                query_rope,
                w_key,
            )

        piece = pl.pallas_call(
            functools.partial(pack_kernel, share=share),
            out_shape=jax.ShapeDtypeStruct((tokens + rope_rows, columns), BF16),
            in_specs=[HBM, HBM],
            out_specs=VMEM,
            scratch_shapes=[
                pltpu.VMEM((share, ROPE), BF16),
                pltpu.SemaphoreType.DMA((2,)),
            ],
            compiler_params=pltpu.CompilerParams(vmem_limit_bytes=2 * MIB),
            name="pack",
        )(kv_latent, key_rope)

        stack = piece[None]
        phases = [("ctx", m, ctx_size) for m in ctx_masks]
        phases += [("head", m, head_size) for m in head_masks]
        done = {}
        for number, phase in enumerate(phases):
            before = stack
            stack = double(stack, *phase)
            if number == 0:
                first, *tables = absorb(before, 0, None)
                stack, first = lax.optimization_barrier((stack, first))
            elif number == 1:
                second = absorb(before, half, tables)
                stack, second = lax.optimization_barrier((stack, second))
            elif number == 2:
                table = jax.ShapeDtypeStruct((ctx_size, head_size * rope_rows, LANES), F32)
                bias = jax.ShapeDtypeStruct((blocks, tokens, chunks_per_block * tokens), F32)
                cosine, sine, bias = pl.pallas_call(
                    functools.partial(
                        table_kernel, ctx_masks=ctx_masks, tokens=tokens, share=share
                    ),
                    out_shape=(table, table, bias),
                    in_specs=[ANY, HBM],
                    out_specs=(VMEM, VMEM, VMEM),
                    scratch_shapes=[
                        pltpu.SMEM(block_order.shape, jnp.int32),
                        pltpu.SemaphoreType.DMA((1,)),
                    ],
                    compiler_params=pltpu.CompilerParams(vmem_limit_bytes=8 * MIB),
                    name="tables",
                )(before, block_order)
                stack, cosine, sine, bias = lax.optimization_barrier((stack, cosine, sine, bias))

        keys = ctx_size * tokens
        scratch = [
            pltpu.VMEM((keys, latent_width + LANES), BF16),
            pltpu.VMEM((tokens, heads * VALUE_DIM), BF16),
            pltpu.SemaphoreType.DMA((heads // group,)),
        ]
        if blocks > 1:
            scratch += [
                pltpu.VMEM((group * tokens, LANES), F32),
                pltpu.VMEM((group * tokens, LANES), F32),
                pltpu.VMEM((group * tokens, latent_width), F32),
            ]
        return pl.pallas_call(
            functools.partial(attend_kernel, head_masks=head_masks, share=share, group=group),
            out_shape=jax.ShapeDtypeStruct((tokens, heads * VALUE_DIM), BF16),
            in_specs=[VMEM] * 8,
            out_specs=HBM,
            scratch_shapes=scratch,
            compiler_params=pltpu.CompilerParams(vmem_limit_bytes=24 * MIB),
            name="attend",
        )(
            stack,
            first,
            second,
            cosine,
            sine,
            bias,
            latent_gain.reshape(1, latent_width),
            w_value,
        )

    return per_device


def solution(mesh):
    return jax.shard_map(
        make_per_device(mesh.shape["ctx"], mesh.shape["head"]),
        mesh=mesh,
        in_specs=(
            P(("group", "ctx"), "head"),
            P(("group", "ctx"), "head"),
            P(("group", "ctx"), "head"),
            P(("group", "ctx"), None),
            P(),
            P(None, "head"),
            P(None, "head"),
            P("group"),
        ),
        out_specs=P(("group", "ctx"), "head"),
        check_vma=False,
    )
```

```python
import functools
import math

import jax
import jax.numpy as jnp
from jax import lax
from jax.experimental import pallas as pl
from jax.experimental.pallas import tpu as pltpu
from jax.sharding import PartitionSpec as P

ROPE = 64
NOPE = 128
VALUE_DIM = 128
LANES = 128

EPSILON = 1e-06
NEGATIVE = -1e30
SCALE = math.log2(math.e) / math.sqrt(NOPE + ROPE)


BF16 = jnp.bfloat16
F32 = jnp.float32
VMEM = pl.BlockSpec(memory_space=pltpu.VMEM)
ANY = pl.BlockSpec(memory_space=pl.ANY)
HBM = pl.BlockSpec(memory_space=pltpu.MemorySpace.HBM)
MIB = 1 << 20


def same_chip(one, other):
    place = getattr(one, "coords", None)
    return place is not None and one.id != other.id and place == getattr(other, "coords", None)


def exchange_masks(mesh):
    sizes = mesh.shape["ctx"], mesh.shape["head"]
    devices = mesh.devices.transpose([mesh.axis_names.index(n) for n in ("group", "ctx", "head")])
    core = None
    for axis, bit in ((1, (1, 0)), (2, (0, 1))):
        if sizes[axis - 1] > 1 and same_chip(devices[0, 0, 0], devices[(0, *bit)]):
            core = bit
    masks = []
    for axis, size in enumerate(sizes):
        while size > 1:
            size //= 2
            mask = (size, 0) if axis == 0 else (0, size)
            if mask != core:
                masks.append(mask)
    if core is not None:
        masks = [(c ^ core[0], h ^ core[1]) for c, h in masks] + [core]
    return masks


def stack_columns(masks, sizes):
    index_of = {(0, 0): 0}
    for bit, (c, h) in enumerate(masks):
        index_of |= {(i ^ c, j ^ h): at ^ (1 << bit) for (i, j), at in index_of.items()}
    ctx_bits = range(sizes[0].bit_length() - 1)
    head_bits = range(sizes[1].bit_length() - 1)
    return [index_of[1 << b, 0] for b in ctx_bits], [index_of[0, 1 << b] for b in head_bits]


def combine(offset, columns):
    index = 0
    for bit, column in enumerate(columns):
        index = index ^ (((offset >> bit) & 1) * column)
    return index


def swap_halves(values):
    half = ROPE // 2
    lane = lax.broadcasted_iota(jnp.int32, values.shape, 1)
    width = values.shape[1]
    return jnp.where(
        lane % ROPE < half, pltpu.roll(values, width - half, 1), pltpu.roll(values, half, 1)
    )


def rotation_tables(place):
    half = ROPE // 2
    lane = lax.broadcasted_iota(jnp.int32, place.shape, 1)
    frequency = jnp.exp(-math.log(10000.0) * (lane % half).astype(F32) / half)
    angle = place.astype(F32) * frequency
    sine = jnp.sin(angle)
    return jnp.cos(angle), jnp.where(lane % ROPE < half, -sine, sine)


def places_of(token, early, late, block_rows):
    return jnp.where(token < block_rows, early, late) * block_rows + token % block_rows


def pack_kernel(latent_hbm, rope_hbm, piece_ref, rope_ref, sems, *, share):
    tokens = latent_hbm.shape[0]
    fold = LANES // ROPE
    rows = share // fold
    first = pl.multiple_of(lax.axis_index("head") * share, share)
    latent_copy = pltpu.make_async_copy(latent_hbm, piece_ref.at[pl.ds(0, tokens)], sems.at[0])
    rope_copy = pltpu.make_async_copy(rope_hbm.at[pl.ds(first, share)], rope_ref, sems.at[1])
    latent_copy.start()
    rope_copy.start()
    rope_copy.wait()
    mine = rope_ref[...].astype(F32)
    parts = [mine[f * rows : (f + 1) * rows] for f in range(fold)]
    piece_ref[tokens:] = jnp.concatenate(parts, 1).astype(BF16)
    latent_copy.wait()


def load_kernel(_, *refs):
    count = len(refs) // 2
    sems = refs[2 * count]
    copies = [
        pltpu.make_async_copy(refs[i], refs[count + i], sems.at[i]) for i in range(count)
    ]
    for copy in copies:
        copy.start()
    for copy in copies:
        copy.wait()


def absorb_kernel(cos_ref, sin_ref, nope_ref, rope_ref, w_key_ref, query_ref):
    tokens = nope_ref.shape[0]
    latent_width = w_key_ref.shape[0]
    heads = w_key_ref.shape[1] // NOPE
    fold = LANES // ROPE
    for head in range(heads):
        columns = slice(head * NOPE, (head + 1) * NOPE)
        absorbed = lax.dot_general(
            nope_ref[:, columns],
            w_key_ref[:, columns],
            (((1,), (1,)), ((), ())),
            preferred_element_type=F32,
        )
        query_ref[head * tokens : (head + 1) * tokens, :latent_width] = absorbed.astype(BF16)
    lane = lax.broadcasted_iota(jnp.int32, (tokens, LANES), 1)
    for pair in range(heads // fold):
        values = rope_ref[:, pair * LANES : (pair + 1) * LANES].astype(F32)
        rotated = values * cos_ref[...] + swap_halves(values) * sin_ref[...]
        for f in range(fold):
            head = pair * fold + f
            kept = jnp.where(lane // ROPE == f, rotated, 0.0)
            query_ref[head * tokens : (head + 1) * tokens, latent_width:] = kept.astype(BF16)


def table_kernel(
    _,
    order_hbm,
    query_cos_ref,
    query_sin_ref,
    cos_ref,
    sin_ref,
    bias_ref,
    order_ref,
    sem,
    *,
    share,
):
    tokens = query_cos_ref.shape[0]
    fold = LANES // ROPE
    rows = share // fold
    block_rows = tokens // 2
    ctx_count, table_rows, _ = cos_ref.shape
    order_copy = pltpu.make_async_copy(order_hbm, order_ref, sem.at[0])
    order_copy.start()
    order_copy.wait()
    ctx_here = lax.axis_index("ctx")
    early = order_ref[2 * ctx_here]
    late = order_ref[2 * ctx_here + 1]
    query_token = lax.broadcasted_iota(jnp.int32, (tokens, LANES), 0)
    query_cos_ref[...], query_sin_ref[...] = rotation_tables(
        places_of(query_token, early, late, block_rows)
    )
    row = lax.broadcasted_iota(jnp.int32, (table_rows, LANES), 0)
    lane = lax.broadcasted_iota(jnp.int32, (table_rows, LANES), 1)
    token = (row // rows) * share + (lane // ROPE) * rows + row % rows
    blocks, _, block = bias_ref.shape
    chunks_per_block = block // tokens
    query_token = lax.broadcasted_iota(jnp.int32, (tokens, block), 0)
    query_place = places_of(query_token, early, late, block_rows)
    key_lane = lax.broadcasted_iota(jnp.int32, (tokens, block), 1)

    def one(b, unused):
        key_place = None
        for i in range(chunks_per_block):
            c = b * chunks_per_block + i
            source = ctx_here ^ c
            early = order_ref[2 * source]
            late = order_ref[2 * source + 1]
            cos_ref[c], sin_ref[c] = rotation_tables(places_of(token, early, late, block_rows))
            place = places_of(key_lane % tokens, early, late, block_rows)
            key_place = place if i == 0 else jnp.where(key_lane < i * tokens, key_place, place)
        bias_ref[b] = jnp.where(key_place <= query_place, 0.0, NEGATIVE)
        return unused

    if blocks == 1:
        one(0, 0)
    else:
        lax.fori_loop(0, blocks, one, 0)


def attend_kernel(
    stack_ref,
    query_ref,
    cos_ref,
    sin_ref,
    bias_ref,
    gain_ref,
    w_value_ref,
    out_hbm,
    key_ref,
    out_ref,
    sems,
    *run_refs,
    ctx_columns,
    head_columns,
    share,
    group,
):
    tokens = bias_ref.shape[1]
    columns = stack_ref.shape[2]
    latent_width = w_value_ref.shape[0]
    heads = w_value_ref.shape[1] // VALUE_DIM
    ctx_count = cos_ref.shape[0]
    head_count = latent_width // columns
    fold = LANES // ROPE
    rope_rows = share // fold
    groups = heads // group
    height = group * tokens
    head_here = lax.axis_index("head")
    places = [combine(head_here ^ h, head_columns) for h in range(head_count)]
    lane = lax.broadcasted_iota(jnp.int32, (rope_rows, LANES), 1)

    def one_chunk(c, unused):
        first = c * tokens
        if not isinstance(c, int):
            first = pl.multiple_of(first, tokens)
        rows = pl.ds(first, tokens)
        here = combine(c, ctx_columns)
        parts = [stack_ref[p ^ here, :tokens, :].astype(F32) for p in places]
        square = functools.reduce(jnp.add, [x * x for x in parts])
        mean = jnp.sum(square, axis=1, keepdims=True) * (1.0 / latent_width)
        factor = lax.rsqrt(mean + EPSILON)
        for h, x in enumerate(parts):
            gain = gain_ref[:, h * columns : (h + 1) * columns]
            key_ref[rows, h * columns : (h + 1) * columns] = (x * factor * gain).astype(BF16)
        pieces = []
        for h, p in enumerate(places):
            values = stack_ref[p ^ here, tokens:, :].astype(F32)
            table = slice(h * rope_rows, (h + 1) * rope_rows)
            values = values * cos_ref[c, table] + swap_halves(values) * sin_ref[c, table]
            turned = pltpu.roll(values, ROPE, 1)
            pieces.append(jnp.where(lane < ROPE, values, turned))
            pieces.append(jnp.where(lane < ROPE, turned, values))
        key_ref[rows, latent_width:] = jnp.concatenate(pieces, 0).astype(BF16)
        return unused

    if ctx_count <= 8:
        for c in range(ctx_count):
            one_chunk(c, 0)
    else:
        lax.fori_loop(0, ctx_count, one_chunk, 0)

    def query_of(g):
        return query_ref[g * height : (g + 1) * height, :]

    def scores_of(query, keys):
        return lax.dot_general(query, keys, (((1,), (1,)), ((), ())), preferred_element_type=F32)

    def masked(scores, b):
        return scores.reshape(group, tokens, -1) * SCALE + bias_ref[b][None]

    def out_copy(g):
        where = pl.ds(g * group * VALUE_DIM, group * VALUE_DIM)
        return pltpu.make_async_copy(out_ref.at[:, where], out_hbm.at[:, where], sems.at[g])

    def finish(g, mixed, total):
        mixed = (mixed * (1.0 / total)).astype(BF16)
        for i in range(group):
            head = g * group + i
            where = slice(head * VALUE_DIM, (head + 1) * VALUE_DIM)
            out_ref[:, where] = jnp.dot(
                mixed[i * tokens : (i + 1) * tokens],
                w_value_ref[:, where],
                preferred_element_type=F32,
            ).astype(BF16)
        out_copy(g).start()

    if bias_ref.shape[0] == 1:
        scores = scores_of(query_of(0), key_ref[...])
        for g in range(groups):
            now = masked(scores, 0)
            if g + 1 < groups:
                scores = scores_of(query_of(g + 1), key_ref[...])
            exps = jnp.exp2(now - jnp.max(now, axis=2, keepdims=True))
            total = jnp.sum(exps, axis=2, keepdims=True).reshape(height, 1)
            mixed = jnp.dot(
                exps.reshape(height, -1).astype(BF16),
                key_ref[:, :latent_width],
                preferred_element_type=F32,
            )
            finish(g, mixed, total)
    else:
        max_ref, total_ref, mixed_ref = run_refs
        block = bias_ref.shape[2]
        for g in range(groups):
            max_ref[...] = jnp.full(max_ref.shape, NEGATIVE, F32)
            total_ref[...] = jnp.zeros(total_ref.shape, F32)
            mixed_ref[...] = jnp.zeros(mixed_ref.shape, F32)
            query = query_of(g)

            def one_block(b, unused):
                keys = key_ref[pl.ds(pl.multiple_of(b * block, block), block), :]
                now = masked(scores_of(query, keys), b)
                old = max_ref[:, :1].reshape(group, tokens, 1)
                new = jnp.maximum(old, jnp.max(now, axis=2, keepdims=True))
                exps = jnp.where(bias_ref[b][None] < 0.0, 0.0, jnp.exp2(now - new))
                shrink = jnp.exp2(old - new).reshape(height, 1)
                total = jnp.sum(exps, axis=2, keepdims=True).reshape(height, 1)
                max_ref[...] = jnp.broadcast_to(new.reshape(height, 1), max_ref.shape)
                total_ref[...] = total_ref[...] * shrink + total
                mixed_ref[...] = mixed_ref[...] * shrink + jnp.dot(
                    exps.reshape(height, block).astype(BF16),
                    keys[:, :latent_width],
                    preferred_element_type=F32,
                )
                return unused

            lax.fori_loop(0, bias_ref.shape[0], one_block, 0)
            finish(g, mixed_ref[...], total_ref[:, :1])
    for g in range(groups):
        out_copy(g).wait()


def make_per_device(sizes, masks):
    ctx_size, head_size = sizes
    ctx_columns, head_columns = stack_columns(masks, sizes)
    everyone = [(c, h) for c in range(ctx_size) for h in range(head_size)]

    def double(stack, mask):
        pairs = [
            (c * head_size + h, (c ^ mask[0]) * head_size + (h ^ mask[1])) for c, h in everyone
        ]
        return jnp.concatenate([stack, lax.ppermute(stack, ("ctx", "head"), pairs)], 0)

    def per_device(
        query_nope, query_rope, kv_latent, key_rope, latent_gain, w_key, w_value, block_order
    ):
        tokens, columns = kv_latent.shape
        heads = w_key.shape[1] // NOPE
        latent_width = w_key.shape[0]
        query_nope, query_rope, kv_latent, key_rope, w_key, block_order = (
            pltpu.with_memory_space_constraint(x, pltpu.MemorySpace.HBM)
            for x in (query_nope, query_rope, kv_latent, key_rope, w_key, block_order)
        )
        share = tokens // head_size
        rope_rows = share * ROPE // LANES
        group = min(4, heads)
        chunks_per_block = min(ctx_size, max(1, 256 // tokens))
        blocks = ctx_size // chunks_per_block

        def tables(after):
            query_table = jax.ShapeDtypeStruct((tokens, LANES), F32)
            table = jax.ShapeDtypeStruct((ctx_size, head_size * rope_rows, LANES), F32)
            bias = jax.ShapeDtypeStruct((blocks, tokens, chunks_per_block * tokens), F32)
            return pl.pallas_call(
                functools.partial(table_kernel, share=share),
                out_shape=(query_table, query_table, table, table, bias),
                in_specs=[ANY, HBM],
                out_specs=(VMEM,) * 5,
                scratch_shapes=[
                    pltpu.SMEM(block_order.shape, jnp.int32),
                    pltpu.SemaphoreType.DMA((1,)),
                ],
                compiler_params=pltpu.CompilerParams(vmem_limit_bytes=8 * MIB),
                name="tables",
            )(after, block_order)

        def load(after, *arrays):
            return pl.pallas_call(
                load_kernel,
                out_shape=[jax.ShapeDtypeStruct(x.shape, x.dtype) for x in arrays],
                in_specs=[ANY] + [HBM] * len(arrays),
                out_specs=[VMEM] * len(arrays),
                scratch_shapes=[pltpu.SemaphoreType.DMA((len(arrays),))],
                compiler_params=pltpu.CompilerParams(vmem_limit_bytes=MIB),
                name="load",
            )(after, *arrays)

        def absorb(*arrays):
            return pl.pallas_call(
                absorb_kernel,
                out_shape=jax.ShapeDtypeStruct((heads * tokens, latent_width + LANES), BF16),
                in_specs=[VMEM] * 5,
                out_specs=VMEM,
                compiler_params=pltpu.CompilerParams(vmem_limit_bytes=8 * MIB),
                name="absorb",
            )(*arrays)

        piece = pl.pallas_call(
            functools.partial(pack_kernel, share=share),
            out_shape=jax.ShapeDtypeStruct((tokens + rope_rows, columns), BF16),
            in_specs=[HBM, HBM],
            out_specs=VMEM,
            scratch_shapes=[
                pltpu.VMEM((share, ROPE), BF16),
                pltpu.SemaphoreType.DMA((2,)),
            ],
            compiler_params=pltpu.CompilerParams(vmem_limit_bytes=2 * MIB),
            name="pack",
        )(kv_latent, key_rope)

        stack = piece[None]
        for number, mask in enumerate(masks):
            before = stack
            stack = double(stack, mask)
            if number == len(masks) - 4:
                stack, *loaded = lax.optimization_barrier(
                    (stack, *load(before, query_nope, query_rope, w_key))
                )
            elif number == len(masks) - 3:
                stack, query_cos, query_sin, cosine, sine, bias = lax.optimization_barrier(
                    (stack, *tables(before))
                )
            elif number == len(masks) - 2:
                *loaded, _ = lax.optimization_barrier((*loaded, before))
                query = absorb(query_cos, query_sin, *loaded)
                stack, query = lax.optimization_barrier((stack, query))

        keys = ctx_size * tokens
        scratch = [
            pltpu.VMEM((keys, latent_width + LANES), BF16),
            pltpu.VMEM((tokens, heads * VALUE_DIM), BF16),
            pltpu.SemaphoreType.DMA((heads // group,)),
        ]
        if blocks > 1:
            scratch += [
                pltpu.VMEM((group * tokens, LANES), F32),
                pltpu.VMEM((group * tokens, LANES), F32),
                pltpu.VMEM((group * tokens, latent_width), F32),
            ]
        return pl.pallas_call(
            functools.partial(
                attend_kernel,
                ctx_columns=ctx_columns,
                head_columns=head_columns,
                share=share,
                group=group,
            ),
            out_shape=jax.ShapeDtypeStruct((tokens, heads * VALUE_DIM), BF16),
            in_specs=[VMEM] * 7,
            out_specs=HBM,
            scratch_shapes=scratch,
            compiler_params=pltpu.CompilerParams(vmem_limit_bytes=24 * MIB),
            name="attend",
        )(stack, query, cosine, sine, bias, latent_gain.reshape(1, latent_width), w_value)

    return per_device


def solution(mesh):
    sizes = mesh.shape["ctx"], mesh.shape["head"]
    return jax.shard_map(
        make_per_device(sizes, exchange_masks(mesh)),
        mesh=mesh,
        in_specs=(
            P(("group", "ctx"), "head"),
            P(("group", "ctx"), "head"),
            P(("group", "ctx"), "head"),
            P(("group", "ctx"), None),
            P(),
            P(None, "head"),
            P(None, "head"),
            P("group"),
        ),
        out_specs=P(("group", "ctx"), "head"),
        check_vma=False,
    )
```

```python
import functools
import math

import jax
import jax.numpy as jnp
from jax import lax
from jax.experimental import pallas as pl
from jax.experimental.pallas import tpu as pltpu
from jax.sharding import PartitionSpec as P

ROPE = 64
NOPE = 128
VALUE_DIM = 128
LANES = 128

EPSILON = 1e-06
NEGATIVE = -1e30
SCALE = math.log2(math.e) / math.sqrt(NOPE + ROPE)


BF16 = jnp.bfloat16
F32 = jnp.float32
VMEM = pl.BlockSpec(memory_space=pltpu.VMEM)
ANY = pl.BlockSpec(memory_space=pl.ANY)
HBM = pl.BlockSpec(memory_space=pltpu.MemorySpace.HBM)
MIB = 1 << 20


def same_chip(one, other):
    place = getattr(one, "coords", None)
    return place is not None and one.id != other.id and place == getattr(other, "coords", None)


def exchange_masks(mesh):
    sizes = mesh.shape["ctx"], mesh.shape["head"]
    devices = mesh.devices.transpose([mesh.axis_names.index(n) for n in ("group", "ctx", "head")])
    core = None
    for axis, bit in ((1, (1, 0)), (2, (0, 1))):
        if sizes[axis - 1] > 1 and same_chip(devices[0, 0, 0], devices[(0, *bit)]):
            core = bit
    masks = []
    for axis, size in enumerate(sizes):
        while size > 1:
            size //= 2
            mask = (size, 0) if axis == 0 else (0, size)
            if mask != core:
                masks.append(mask)
    if core is not None:
        masks = [(c ^ core[0], h ^ core[1]) for c, h in masks] + [core]
    return masks


def stack_columns(masks, sizes):
    index_of = {(0, 0): 0}
    for bit, (c, h) in enumerate(masks):
        index_of |= {(i ^ c, j ^ h): at ^ (1 << bit) for (i, j), at in index_of.items()}
    ctx_bits = range(sizes[0].bit_length() - 1)
    head_bits = range(sizes[1].bit_length() - 1)
    return [index_of[1 << b, 0] for b in ctx_bits], [index_of[0, 1 << b] for b in head_bits]


def combine(offset, columns):
    index = 0
    for bit, column in enumerate(columns):
        index = index ^ (((offset >> bit) & 1) * column)
    return index


def swap_halves(values):
    half = ROPE // 2
    lane = lax.broadcasted_iota(jnp.int32, values.shape, 1)
    width = values.shape[1]
    return jnp.where(
        lane % ROPE < half, pltpu.roll(values, width - half, 1), pltpu.roll(values, half, 1)
    )


def rotation_tables(place):
    half = ROPE // 2
    lane = lax.broadcasted_iota(jnp.int32, place.shape, 1)
    frequency = jnp.exp(-math.log(10000.0) * (lane % half).astype(F32) / half)
    angle = place.astype(F32) * frequency
    sine = jnp.sin(angle)
    return jnp.cos(angle), jnp.where(lane % ROPE < half, -sine, sine)


def places_of(token, early, late, block_rows):
    return jnp.where(token < block_rows, early, late) * block_rows + token % block_rows


def pack_kernel(latent_hbm, rope_hbm, piece_ref, rope_ref, sems, *, share):
    tokens = latent_hbm.shape[0]
    fold = LANES // ROPE
    rows = share // fold
    first = pl.multiple_of(lax.axis_index("head") * share, share)
    latent_copy = pltpu.make_async_copy(latent_hbm, piece_ref.at[pl.ds(0, tokens)], sems.at[0])
    rope_copy = pltpu.make_async_copy(rope_hbm.at[pl.ds(first, share)], rope_ref, sems.at[1])
    latent_copy.start()
    rope_copy.start()
    rope_copy.wait()
    mine = rope_ref[...].astype(F32)
    parts = [mine[f * rows : (f + 1) * rows] for f in range(fold)]
    piece_ref[tokens:] = jnp.concatenate(parts, 1).astype(BF16)
    latent_copy.wait()


def load_kernel(_, nope_hbm, w_key_hbm, nope_ref, top_ref, sems):
    top_copy = pltpu.make_async_copy(
        w_key_hbm.at[pl.ds(0, top_ref.shape[0])], top_ref, sems.at[0]
    )
    nope_copy = pltpu.make_async_copy(nope_hbm, nope_ref, sems.at[1])
    top_copy.start()
    nope_copy.start()
    top_copy.wait()
    nope_copy.wait()


def absorb_kernel(cos_ref, sin_ref, nope_ref, rope_ref, top_ref, bottom_ref, query_ref):
    tokens = nope_ref.shape[0]
    part = top_ref.shape[0]
    heads = top_ref.shape[1] // NOPE
    fold = LANES // ROPE
    for head in range(heads):
        columns = slice(head * NOPE, (head + 1) * NOPE)
        for i, w_key_ref in enumerate((top_ref, bottom_ref)):
            absorbed = lax.dot_general(
                nope_ref[:, columns],
                w_key_ref[:, columns],
                (((1,), (1,)), ((), ())),
                preferred_element_type=F32,
            )
            query_ref[head * tokens : (head + 1) * tokens, i * part : (i + 1) * part] = (
                absorbed.astype(BF16)
            )
    lane = lax.broadcasted_iota(jnp.int32, (tokens, LANES), 1)
    for pair in range(heads // fold):
        values = rope_ref[:, pair * LANES : (pair + 1) * LANES].astype(F32)
        rotated = values * cos_ref[...] + swap_halves(values) * sin_ref[...]
        for f in range(fold):
            head = pair * fold + f
            kept = jnp.where(lane // ROPE == f, rotated, 0.0)
            query_ref[head * tokens : (head + 1) * tokens, 2 * part :] = kept.astype(BF16)


def table_kernel(
    _,
    order_hbm,
    rope_hbm,
    w_key_hbm,
    query_cos_ref,
    query_sin_ref,
    cos_ref,
    sin_ref,
    bias_ref,
    rope_ref,
    bottom_ref,
    order_ref,
    sems,
    *,
    share,
):
    tokens = query_cos_ref.shape[0]
    part = bottom_ref.shape[0]
    fold = LANES // ROPE
    rows = share // fold
    block_rows = tokens // 2
    ctx_count, table_rows, _ = cos_ref.shape
    order_copy = pltpu.make_async_copy(order_hbm, order_ref, sems.at[0])
    rope_copy = pltpu.make_async_copy(rope_hbm, rope_ref, sems.at[1])
    bottom_copy = pltpu.make_async_copy(
        w_key_hbm.at[pl.ds(w_key_hbm.shape[0] - part, part)], bottom_ref, sems.at[2]
    )
    order_copy.start()
    bottom_copy.start()
    rope_copy.start()
    order_copy.wait()
    ctx_here = lax.axis_index("ctx")
    early = order_ref[2 * ctx_here]
    late = order_ref[2 * ctx_here + 1]
    query_token = lax.broadcasted_iota(jnp.int32, (tokens, LANES), 0)
    query_cos_ref[...], query_sin_ref[...] = rotation_tables(
        places_of(query_token, early, late, block_rows)
    )
    row = lax.broadcasted_iota(jnp.int32, (table_rows, LANES), 0)
    lane = lax.broadcasted_iota(jnp.int32, (table_rows, LANES), 1)
    token = (row // rows) * share + (lane // ROPE) * rows + row % rows
    blocks, _, block = bias_ref.shape
    chunks_per_block = block // tokens
    query_token = lax.broadcasted_iota(jnp.int32, (tokens, block), 0)
    query_place = places_of(query_token, early, late, block_rows)
    key_lane = lax.broadcasted_iota(jnp.int32, (tokens, block), 1)

    def one(b, unused):
        key_place = None
        for i in range(chunks_per_block):
            c = b * chunks_per_block + i
            source = ctx_here ^ c
            early = order_ref[2 * source]
            late = order_ref[2 * source + 1]
            cos_ref[c], sin_ref[c] = rotation_tables(places_of(token, early, late, block_rows))
            place = places_of(key_lane % tokens, early, late, block_rows)
            key_place = place if i == 0 else jnp.where(key_lane < i * tokens, key_place, place)
        bias_ref[b] = jnp.where(key_place <= query_place, 0.0, NEGATIVE)
        return unused

    if blocks == 1:
        one(0, 0)
    else:
        lax.fori_loop(0, blocks, one, 0)
    rope_copy.wait()
    bottom_copy.wait()


def attend_kernel(
    stack_ref,
    query_ref,
    cos_ref,
    sin_ref,
    bias_ref,
    gain_ref,
    w_value_ref,
    out_hbm,
    key_ref,
    out_ref,
    sems,
    *run_refs,
    ctx_columns,
    head_columns,
    share,
    groups,
    ahead,
):
    tokens = bias_ref.shape[1]
    columns = stack_ref.shape[2]
    latent_width = w_value_ref.shape[0]
    heads = w_value_ref.shape[1] // VALUE_DIM
    ctx_count = cos_ref.shape[0]
    head_count = latent_width // columns
    fold = LANES // ROPE
    rope_rows = share // fold
    starts = [sum(groups[:g]) for g in range(len(groups))]
    head_here = lax.axis_index("head")
    places = [combine(head_here ^ h, head_columns) for h in range(head_count)]
    lane = lax.broadcasted_iota(jnp.int32, (rope_rows, LANES), 1)

    def one_chunk(c, unused):
        first = c * tokens
        if not isinstance(c, int):
            first = pl.multiple_of(first, tokens)
        rows = pl.ds(first, tokens)
        here = combine(c, ctx_columns)
        parts = [stack_ref[p ^ here, :tokens, :].astype(F32) for p in places]
        square = functools.reduce(jnp.add, [x * x for x in parts])
        mean = jnp.sum(square, axis=1, keepdims=True) * (1.0 / latent_width)
        factor = lax.rsqrt(mean + EPSILON)
        for h, x in enumerate(parts):
            gain = gain_ref[:, h * columns : (h + 1) * columns]
            key_ref[rows, h * columns : (h + 1) * columns] = (x * factor * gain).astype(BF16)
        pieces = []
        for h, p in enumerate(places):
            values = stack_ref[p ^ here, tokens:, :].astype(F32)
            table = slice(h * rope_rows, (h + 1) * rope_rows)
            values = values * cos_ref[c, table] + swap_halves(values) * sin_ref[c, table]
            turned = pltpu.roll(values, ROPE, 1)
            pieces.append(jnp.where(lane < ROPE, values, turned))
            pieces.append(jnp.where(lane < ROPE, turned, values))
        key_ref[rows, latent_width:] = jnp.concatenate(pieces, 0).astype(BF16)
        return unused

    if ctx_count <= 8:
        for c in range(ctx_count):
            one_chunk(c, 0)
    else:
        lax.fori_loop(0, ctx_count, one_chunk, 0)

    def scores_of(g, keys):
        first = starts[g] * tokens
        query = query_ref[first : first + groups[g] * tokens, :]
        return lax.dot_general(query, keys, (((1,), (1,)), ((), ())), preferred_element_type=F32)

    def masked(scores, b):
        return scores.reshape(-1, tokens, scores.shape[1]) * SCALE + bias_ref[b][None]

    def out_copy(g):
        where = pl.ds(starts[g] * VALUE_DIM, groups[g] * VALUE_DIM)
        return pltpu.make_async_copy(out_ref.at[:, where], out_hbm.at[:, where], sems.at[g])

    def finish(g, mixed, total):
        mixed = (mixed * (1.0 / total)).astype(BF16)
        for i in range(groups[g]):
            head = starts[g] + i
            where = slice(head * VALUE_DIM, (head + 1) * VALUE_DIM)
            out_ref[:, where] = jnp.dot(
                mixed[i * tokens : (i + 1) * tokens],
                w_value_ref[:, where],
                preferred_element_type=F32,
            ).astype(BF16)
        out_copy(g).start()

    if bias_ref.shape[0] == 1:
        scores = [scores_of(g, key_ref[...]) for g in range(min(ahead, len(groups)))]
        for g in range(len(groups)):
            now = masked(scores[g], 0)
            if g + ahead < len(groups):
                scores.append(scores_of(g + ahead, key_ref[...]))
            exps = jnp.exp2(now - jnp.max(now, axis=2, keepdims=True))
            total = jnp.sum(exps, axis=2, keepdims=True).reshape(-1, 1)
            mixed = jnp.dot(
                exps.reshape(-1, exps.shape[2]).astype(BF16),
                key_ref[:, :latent_width],
                preferred_element_type=F32,
            )
            finish(g, mixed, total)
    else:
        max_ref, total_ref, mixed_ref = run_refs
        block = bias_ref.shape[2]
        for g, group in enumerate(groups):
            height = group * tokens
            rows = slice(0, height)
            max_ref[rows] = jnp.full((height, LANES), NEGATIVE, F32)
            total_ref[rows] = jnp.zeros((height, LANES), F32)
            mixed_ref[rows] = jnp.zeros((height, latent_width), F32)

            def one_block(b, unused):
                keys = key_ref[pl.ds(pl.multiple_of(b * block, block), block), :]
                now = masked(scores_of(g, keys), b)
                old = max_ref[rows, :1].reshape(group, tokens, 1)
                new = jnp.maximum(old, jnp.max(now, axis=2, keepdims=True))
                exps = jnp.where(bias_ref[b][None] < 0.0, 0.0, jnp.exp2(now - new))
                shrink = jnp.exp2(old - new).reshape(height, 1)
                total = jnp.sum(exps, axis=2, keepdims=True).reshape(height, 1)
                max_ref[rows] = jnp.broadcast_to(new.reshape(height, 1), (height, LANES))
                total_ref[rows] = total_ref[rows] * shrink + total
                mixed_ref[rows] = mixed_ref[rows] * shrink + jnp.dot(
                    exps.reshape(height, block).astype(BF16),
                    keys[:, :latent_width],
                    preferred_element_type=F32,
                )
                return unused

            lax.fori_loop(0, bias_ref.shape[0], one_block, 0)
            finish(g, mixed_ref[rows], total_ref[rows, :1])
    for g in range(len(groups)):
        out_copy(g).wait()


def head_groups(heads):
    if heads % 4:
        return [heads]
    return [heads // 4, heads // 2, heads // 4]


def make_per_device(sizes, masks):
    ctx_size, head_size = sizes
    ctx_columns, head_columns = stack_columns(masks, sizes)
    everyone = [(c, h) for c in range(ctx_size) for h in range(head_size)]

    def double(stack, mask):
        pairs = [
            (c * head_size + h, (c ^ mask[0]) * head_size + (h ^ mask[1])) for c, h in everyone
        ]
        return jnp.concatenate([stack, lax.ppermute(stack, ("ctx", "head"), pairs)], 0)

    def per_device(
        query_nope, query_rope, kv_latent, key_rope, latent_gain, w_key, w_value, block_order
    ):
        tokens, columns = kv_latent.shape
        heads = w_key.shape[1] // NOPE
        latent_width = w_key.shape[0]
        query_nope, query_rope, kv_latent, key_rope, w_key, block_order = (
            pltpu.with_memory_space_constraint(x, pltpu.MemorySpace.HBM)
            for x in (query_nope, query_rope, kv_latent, key_rope, w_key, block_order)
        )
        share = tokens // head_size
        rope_rows = share * ROPE // LANES
        groups = head_groups(heads)
        chunks_per_block = min(ctx_size, max(1, 256 // tokens))
        blocks = ctx_size // chunks_per_block

        half_key = jax.ShapeDtypeStruct((latent_width // 2, heads * NOPE), BF16)

        def load(after):
            return pl.pallas_call(
                load_kernel,
                out_shape=(jax.ShapeDtypeStruct((tokens, heads * NOPE), BF16), half_key),
                in_specs=[ANY, HBM, HBM],
                out_specs=(VMEM, VMEM),
                scratch_shapes=[pltpu.SemaphoreType.DMA((2,))],
                compiler_params=pltpu.CompilerParams(vmem_limit_bytes=MIB),
                name="load",
            )(after, query_nope, w_key)

        def tables(after):
            query_table = jax.ShapeDtypeStruct((tokens, LANES), F32)
            table = jax.ShapeDtypeStruct((ctx_size, head_size * rope_rows, LANES), F32)
            bias = jax.ShapeDtypeStruct((blocks, tokens, chunks_per_block * tokens), F32)
            rope = jax.ShapeDtypeStruct((tokens, heads * ROPE), BF16)
            return pl.pallas_call(
                functools.partial(table_kernel, share=share),
                out_shape=(query_table, query_table, table, table, bias, rope, half_key),
                in_specs=[ANY, HBM, HBM, HBM],
                out_specs=(VMEM,) * 7,
                scratch_shapes=[
                    pltpu.SMEM(block_order.shape, jnp.int32),
                    pltpu.SemaphoreType.DMA((3,)),
                ],
                compiler_params=pltpu.CompilerParams(vmem_limit_bytes=8 * MIB),
                name="tables",
            )(after, block_order, query_rope, w_key)

        def absorb(*arrays):
            return pl.pallas_call(
                absorb_kernel,
                out_shape=jax.ShapeDtypeStruct((heads * tokens, latent_width + LANES), BF16),
                in_specs=[VMEM] * 6,
                out_specs=VMEM,
                compiler_params=pltpu.CompilerParams(vmem_limit_bytes=8 * MIB),
                name="absorb",
            )(*arrays)

        piece = pl.pallas_call(
            functools.partial(pack_kernel, share=share),
            out_shape=jax.ShapeDtypeStruct((tokens + rope_rows, columns), BF16),
            in_specs=[HBM, HBM],
            out_specs=VMEM,
            scratch_shapes=[
                pltpu.VMEM((share, ROPE), BF16),
                pltpu.SemaphoreType.DMA((2,)),
            ],
            compiler_params=pltpu.CompilerParams(vmem_limit_bytes=2 * MIB),
            name="pack",
        )(kv_latent, key_rope)

        stack = piece[None]
        for number, mask in enumerate(masks):
            before = stack
            stack = double(stack, mask)
            if number == len(masks) - 4:
                stack, nope, top = lax.optimization_barrier((stack, *load(before)))
            elif number == len(masks) - 3:
                stack, query_cos, query_sin, cosine, sine, bias, rope, bottom = (
                    lax.optimization_barrier((stack, *tables(before)))
                )
            elif number == len(masks) - 2:
                _, *arrays = lax.optimization_barrier(
                    (before, query_cos, query_sin, nope, rope, top, bottom)
                )
                stack, query = lax.optimization_barrier((stack, absorb(*arrays)))

        keys = ctx_size * tokens
        scratch = [
            pltpu.VMEM((keys, latent_width + LANES), BF16),
            pltpu.VMEM((tokens, heads * VALUE_DIM), BF16),
            pltpu.SemaphoreType.DMA((len(groups),)),
        ]
        if blocks > 1:
            scratch += [
                pltpu.VMEM((max(groups) * tokens, LANES), F32),
                pltpu.VMEM((max(groups) * tokens, LANES), F32),
                pltpu.VMEM((max(groups) * tokens, latent_width), F32),
            ]
        return pl.pallas_call(
            functools.partial(
                attend_kernel,
                ctx_columns=ctx_columns,
                head_columns=head_columns,
                share=share,
                groups=groups,
                ahead=2,
            ),
            out_shape=jax.ShapeDtypeStruct((tokens, heads * VALUE_DIM), BF16),
            in_specs=[VMEM] * 7,
            out_specs=HBM,
            scratch_shapes=scratch,
            compiler_params=pltpu.CompilerParams(vmem_limit_bytes=24 * MIB),
            name="attend",
        )(stack, query, cosine, sine, bias, latent_gain.reshape(1, latent_width), w_value)

    return per_device


def solution(mesh):
    sizes = mesh.shape["ctx"], mesh.shape["head"]
    return jax.shard_map(
        make_per_device(sizes, exchange_masks(mesh)),
        mesh=mesh,
        in_specs=(
            P(("group", "ctx"), "head"),
            P(("group", "ctx"), "head"),
            P(("group", "ctx"), "head"),
            P(("group", "ctx"), None),
            P(),
            P(None, "head"),
            P(None, "head"),
            P("group"),
        ),
        out_specs=P(("group", "ctx"), "head"),
        check_vma=False,
    )
```

```python
import functools
import math

import jax
import jax.numpy as jnp
from jax import lax
from jax.experimental import pallas as pl
from jax.experimental.pallas import tpu as pltpu
from jax.sharding import PartitionSpec as P

ROPE = 64
NOPE = 128
VALUE_DIM = 128
LANES = 128

EPSILON = 1e-06
NEGATIVE = -1e30
SCALE = math.log2(math.e) / math.sqrt(NOPE + ROPE)


BF16 = jnp.bfloat16
F32 = jnp.float32
VMEM = pl.BlockSpec(memory_space=pltpu.VMEM)
ANY = pl.BlockSpec(memory_space=pl.ANY)
HBM = pl.BlockSpec(memory_space=pltpu.MemorySpace.HBM)
MIB = 1 << 20


def same_chip(one, other):
    place = getattr(one, "coords", None)
    return place is not None and one.id != other.id and place == getattr(other, "coords", None)


def exchange_masks(mesh):
    sizes = mesh.shape["ctx"], mesh.shape["head"]
    devices = mesh.devices.transpose([mesh.axis_names.index(n) for n in ("group", "ctx", "head")])
    core = None
    for axis, bit in ((1, (1, 0)), (2, (0, 1))):
        if sizes[axis - 1] > 1 and same_chip(devices[0, 0, 0], devices[(0, *bit)]):
            core = bit
    masks = []
    for axis, size in enumerate(sizes):
        while size > 1:
            size //= 2
            mask = (size, 0) if axis == 0 else (0, size)
            if mask != core:
                masks.append(mask)
    if core is not None:
        masks = [(c ^ core[0], h ^ core[1]) for c, h in masks] + [core]
    return masks


def stack_columns(masks, sizes):
    index_of = {(0, 0): 0}
    for bit, (c, h) in enumerate(masks):
        index_of |= {(i ^ c, j ^ h): at ^ (1 << bit) for (i, j), at in index_of.items()}
    ctx_bits = range(sizes[0].bit_length() - 1)
    head_bits = range(sizes[1].bit_length() - 1)
    return [index_of[1 << b, 0] for b in ctx_bits], [index_of[0, 1 << b] for b in head_bits]


def combine(offset, columns):
    index = 0
    for bit, column in enumerate(columns):
        index = index ^ (((offset >> bit) & 1) * column)
    return index


def swap_halves(values):
    half = ROPE // 2
    lane = lax.broadcasted_iota(jnp.int32, values.shape, 1)
    width = values.shape[1]
    return jnp.where(
        lane % ROPE < half, pltpu.roll(values, width - half, 1), pltpu.roll(values, half, 1)
    )


def rotation_tables(place):
    half = ROPE // 2
    lane = lax.broadcasted_iota(jnp.int32, place.shape, 1)
    frequency = jnp.exp(-math.log(10000.0) * (lane % half).astype(F32) / half)
    angle = place.astype(F32) * frequency
    sine = jnp.sin(angle)
    return jnp.cos(angle), jnp.where(lane % ROPE < half, -sine, sine)


def places_of(token, early, late, block_rows):
    return jnp.where(token < block_rows, early, late) * block_rows + token % block_rows


def pack_kernel(latent_hbm, rope_hbm, piece_ref, rope_ref, sems, *, share):
    tokens = latent_hbm.shape[0]
    fold = LANES // ROPE
    rows = share // fold
    first = pl.multiple_of(lax.axis_index("head") * share, share)
    latent_copy = pltpu.make_async_copy(latent_hbm, piece_ref.at[pl.ds(0, tokens)], sems.at[0])
    rope_copy = pltpu.make_async_copy(rope_hbm.at[pl.ds(first, share)], rope_ref, sems.at[1])
    latent_copy.start()
    rope_copy.start()
    rope_copy.wait()
    mine = rope_ref[...].astype(F32)
    parts = [mine[f * rows : (f + 1) * rows] for f in range(fold)]
    piece_ref[tokens:] = jnp.concatenate(parts, 1).astype(BF16)
    latent_copy.wait()


def load_kernel(_, nope_hbm, w_key_hbm, nope_ref, top_ref, sems):
    top_copy = pltpu.make_async_copy(
        w_key_hbm.at[pl.ds(0, top_ref.shape[0])], top_ref, sems.at[0]
    )
    nope_copy = pltpu.make_async_copy(nope_hbm, nope_ref, sems.at[1])
    top_copy.start()
    nope_copy.start()
    top_copy.wait()
    nope_copy.wait()


def absorb_kernel(cos_ref, sin_ref, nope_ref, rope_ref, top_ref, bottom_ref, query_ref):
    tokens = nope_ref.shape[0]
    part = top_ref.shape[0]
    heads = top_ref.shape[1] // NOPE
    fold = LANES // ROPE
    for head in range(heads):
        columns = slice(head * NOPE, (head + 1) * NOPE)
        for i, w_key_ref in enumerate((top_ref, bottom_ref)):
            absorbed = lax.dot_general(
                nope_ref[:, columns],
                w_key_ref[:, columns],
                (((1,), (1,)), ((), ())),
                preferred_element_type=F32,
            )
            query_ref[head * tokens : (head + 1) * tokens, i * part : (i + 1) * part] = (
                absorbed.astype(BF16)
            )
    lane = lax.broadcasted_iota(jnp.int32, (tokens, LANES), 1)
    for pair in range(heads // fold):
        values = rope_ref[:, pair * LANES : (pair + 1) * LANES].astype(F32)
        rotated = values * cos_ref[...] + swap_halves(values) * sin_ref[...]
        for f in range(fold):
            head = pair * fold + f
            kept = jnp.where(lane // ROPE == f, rotated, 0.0)
            query_ref[head * tokens : (head + 1) * tokens, 2 * part :] = kept.astype(BF16)


def table_kernel(
    _,
    order_hbm,
    rope_hbm,
    w_key_hbm,
    query_cos_ref,
    query_sin_ref,
    cos_ref,
    sin_ref,
    bias_ref,
    rope_ref,
    bottom_ref,
    order_ref,
    sems,
    *,
    share,
):
    tokens = query_cos_ref.shape[0]
    part = bottom_ref.shape[0]
    fold = LANES // ROPE
    rows = share // fold
    block_rows = tokens // 2
    ctx_count, table_rows, _ = cos_ref.shape
    order_copy = pltpu.make_async_copy(order_hbm, order_ref, sems.at[0])
    rope_copy = pltpu.make_async_copy(rope_hbm, rope_ref, sems.at[1])
    bottom_copy = pltpu.make_async_copy(
        w_key_hbm.at[pl.ds(w_key_hbm.shape[0] - part, part)], bottom_ref, sems.at[2]
    )
    order_copy.start()
    bottom_copy.start()
    rope_copy.start()
    order_copy.wait()
    ctx_here = lax.axis_index("ctx")
    early = order_ref[2 * ctx_here]
    late = order_ref[2 * ctx_here + 1]
    query_token = lax.broadcasted_iota(jnp.int32, (tokens, LANES), 0)
    query_cos_ref[...], query_sin_ref[...] = rotation_tables(
        places_of(query_token, early, late, block_rows)
    )
    row = lax.broadcasted_iota(jnp.int32, (table_rows, LANES), 0)
    lane = lax.broadcasted_iota(jnp.int32, (table_rows, LANES), 1)
    token = (row // rows) * share + (lane // ROPE) * rows + row % rows
    blocks, _, block = bias_ref.shape
    chunks_per_block = block // tokens
    query_token = lax.broadcasted_iota(jnp.int32, (tokens, block), 0)
    query_place = places_of(query_token, early, late, block_rows)
    key_lane = lax.broadcasted_iota(jnp.int32, (tokens, block), 1)

    def one(b, unused):
        key_place = None
        for i in range(chunks_per_block):
            c = b * chunks_per_block + i
            source = ctx_here ^ c
            early = order_ref[2 * source]
            late = order_ref[2 * source + 1]
            cos_ref[c], sin_ref[c] = rotation_tables(places_of(token, early, late, block_rows))
            place = places_of(key_lane % tokens, early, late, block_rows)
            key_place = place if i == 0 else jnp.where(key_lane < i * tokens, key_place, place)
        bias_ref[b] = jnp.where(key_place <= query_place, 0.0, NEGATIVE)
        return unused

    if blocks == 1:
        one(0, 0)
    else:
        lax.fori_loop(0, blocks, one, 0)
    rope_copy.wait()
    bottom_copy.wait()


def attend_kernel(
    stack_ref,
    query_ref,
    cos_ref,
    sin_ref,
    bias_ref,
    gain_ref,
    w_value_ref,
    out_hbm,
    key_ref,
    out_ref,
    sems,
    *run_refs,
    ctx_columns,
    head_columns,
    share,
    groups,
    ahead,
):
    tokens = bias_ref.shape[1]
    columns = stack_ref.shape[2]
    latent_width = w_value_ref.shape[0]
    heads = w_value_ref.shape[1] // VALUE_DIM
    ctx_count = cos_ref.shape[0]
    head_count = latent_width // columns
    fold = LANES // ROPE
    rope_rows = share // fold
    starts = [sum(groups[:g]) for g in range(len(groups))]
    head_here = lax.axis_index("head")
    places = [combine(head_here ^ h, head_columns) for h in range(head_count)]
    lane = lax.broadcasted_iota(jnp.int32, (rope_rows, LANES), 1)

    def one_chunk(c, unused):
        first = c * tokens
        if not isinstance(c, int):
            first = pl.multiple_of(first, tokens)
        rows = pl.ds(first, tokens)
        here = combine(c, ctx_columns)
        parts = [stack_ref[p ^ here, :tokens, :].astype(F32) for p in places]
        square = functools.reduce(jnp.add, [x * x for x in parts])
        mean = jnp.sum(square, axis=1, keepdims=True) * (1.0 / latent_width)
        factor = lax.rsqrt(mean + EPSILON)
        for h, x in enumerate(parts):
            gain = gain_ref[:, h * columns : (h + 1) * columns]
            key_ref[rows, h * columns : (h + 1) * columns] = (x * factor * gain).astype(BF16)
        pieces = []
        for h, p in enumerate(places):
            values = stack_ref[p ^ here, tokens:, :].astype(F32)
            table = slice(h * rope_rows, (h + 1) * rope_rows)
            values = values * cos_ref[c, table] + swap_halves(values) * sin_ref[c, table]
            turned = pltpu.roll(values, ROPE, 1)
            pieces.append(jnp.where(lane < ROPE, values, turned))
            pieces.append(jnp.where(lane < ROPE, turned, values))
        key_ref[rows, latent_width:] = jnp.concatenate(pieces, 0).astype(BF16)
        return unused

    if ctx_count <= 8:
        for c in range(ctx_count):
            one_chunk(c, 0)
    else:
        lax.fori_loop(0, ctx_count, one_chunk, 0)

    def scores_of(g, keys):
        first = starts[g] * tokens
        query = query_ref[first : first + groups[g] * tokens, :]
        return lax.dot_general(query, keys, (((1,), (1,)), ((), ())), preferred_element_type=F32)

    def masked(scores, b):
        return scores.reshape(-1, tokens, scores.shape[1]) * SCALE + bias_ref[b][None]

    def out_copy(g):
        where = pl.ds(starts[g] * VALUE_DIM, groups[g] * VALUE_DIM)
        return pltpu.make_async_copy(out_ref.at[:, where], out_hbm.at[:, where], sems.at[g])

    def finish(g, mixed, total):
        mixed = (mixed * (1.0 / total)).astype(BF16)
        for i in range(groups[g]):
            head = starts[g] + i
            where = slice(head * VALUE_DIM, (head + 1) * VALUE_DIM)
            out_ref[:, where] = jnp.dot(
                mixed[i * tokens : (i + 1) * tokens],
                w_value_ref[:, where],
                preferred_element_type=F32,
            ).astype(BF16)
        out_copy(g).start()

    if bias_ref.shape[0] == 1:
        scores = [scores_of(g, key_ref[...]) for g in range(min(ahead, len(groups)))]
        for g in range(len(groups)):
            now = masked(scores[g], 0)
            if g + ahead < len(groups):
                scores.append(scores_of(g + ahead, key_ref[...]))
            exps = jnp.exp2(now - jnp.max(now, axis=2, keepdims=True))
            total = jnp.sum(exps, axis=2, keepdims=True).reshape(-1, 1)
            mixed = jnp.dot(
                exps.reshape(-1, exps.shape[2]).astype(BF16),
                key_ref[:, :latent_width],
                preferred_element_type=F32,
            )
            finish(g, mixed, total)
    else:
        max_ref, total_ref, mixed_ref = run_refs
        block = bias_ref.shape[2]
        for g, group in enumerate(groups):
            height = group * tokens
            rows = slice(0, height)
            max_ref[rows] = jnp.full((height, LANES), NEGATIVE, F32)
            total_ref[rows] = jnp.zeros((height, LANES), F32)
            mixed_ref[rows] = jnp.zeros((height, latent_width), F32)

            def one_block(b, unused):
                keys = key_ref[pl.ds(pl.multiple_of(b * block, block), block), :]
                now = masked(scores_of(g, keys), b)
                old = max_ref[rows, :1].reshape(group, tokens, 1)
                new = jnp.maximum(old, jnp.max(now, axis=2, keepdims=True))
                exps = jnp.where(bias_ref[b][None] < 0.0, 0.0, jnp.exp2(now - new))
                shrink = jnp.exp2(old - new).reshape(height, 1)
                total = jnp.sum(exps, axis=2, keepdims=True).reshape(height, 1)
                max_ref[rows] = jnp.broadcast_to(new.reshape(height, 1), (height, LANES))
                total_ref[rows] = total_ref[rows] * shrink + total
                mixed_ref[rows] = mixed_ref[rows] * shrink + jnp.dot(
                    exps.reshape(height, block).astype(BF16),
                    keys[:, :latent_width],
                    preferred_element_type=F32,
                )
                return unused

            lax.fori_loop(0, bias_ref.shape[0], one_block, 0)
            finish(g, mixed_ref[rows], total_ref[rows, :1])
    for g in range(len(groups)):
        out_copy(g).wait()


def head_groups(heads):
    if heads < 3:
        return [heads]
    return [heads // 3, heads - 2 * (heads // 3), heads // 3]


def make_per_device(sizes, masks):
    ctx_size, head_size = sizes
    ctx_columns, head_columns = stack_columns(masks, sizes)
    everyone = [(c, h) for c in range(ctx_size) for h in range(head_size)]

    def exchange(stack, mask):
        pairs = [
            (c * head_size + h, (c ^ mask[0]) * head_size + (h ^ mask[1])) for c, h in everyone
        ]
        return lax.ppermute(stack, ("ctx", "head"), pairs)

    def per_device(
        query_nope, query_rope, kv_latent, key_rope, latent_gain, w_key, w_value, block_order
    ):
        tokens, columns = kv_latent.shape
        heads = w_key.shape[1] // NOPE
        latent_width = w_key.shape[0]
        query_nope, query_rope, kv_latent, key_rope, w_key, block_order = (
            pltpu.with_memory_space_constraint(x, pltpu.MemorySpace.HBM)
            for x in (query_nope, query_rope, kv_latent, key_rope, w_key, block_order)
        )
        share = tokens // head_size
        rope_rows = share * ROPE // LANES
        groups = head_groups(heads)
        chunks_per_block = min(ctx_size, max(1, 256 // tokens))
        blocks = ctx_size // chunks_per_block

        half_key = jax.ShapeDtypeStruct((latent_width // 2, heads * NOPE), BF16)

        def load(after):
            return pl.pallas_call(
                load_kernel,
                out_shape=(jax.ShapeDtypeStruct((tokens, heads * NOPE), BF16), half_key),
                in_specs=[ANY, HBM, HBM],
                out_specs=(VMEM, VMEM),
                scratch_shapes=[pltpu.SemaphoreType.DMA((2,))],
                compiler_params=pltpu.CompilerParams(vmem_limit_bytes=MIB),
                name="load",
            )(after, query_nope, w_key)

        def tables(after):
            query_table = jax.ShapeDtypeStruct((tokens, LANES), F32)
            table = jax.ShapeDtypeStruct((ctx_size, head_size * rope_rows, LANES), F32)
            bias = jax.ShapeDtypeStruct((blocks, tokens, chunks_per_block * tokens), F32)
            rope = jax.ShapeDtypeStruct((tokens, heads * ROPE), BF16)
            return pl.pallas_call(
                functools.partial(table_kernel, share=share),
                out_shape=(query_table, query_table, table, table, bias, rope, half_key),
                in_specs=[ANY, HBM, HBM, HBM],
                out_specs=(VMEM,) * 7,
                scratch_shapes=[
                    pltpu.SMEM(block_order.shape, jnp.int32),
                    pltpu.SemaphoreType.DMA((3,)),
                ],
                compiler_params=pltpu.CompilerParams(vmem_limit_bytes=8 * MIB),
                name="tables",
            )(after, block_order, query_rope, w_key)

        def absorb(*arrays):
            return pl.pallas_call(
                absorb_kernel,
                out_shape=jax.ShapeDtypeStruct((heads * tokens, latent_width + LANES), BF16),
                in_specs=[VMEM] * 6,
                out_specs=VMEM,
                compiler_params=pltpu.CompilerParams(vmem_limit_bytes=8 * MIB),
                name="absorb",
            )(*arrays)

        piece = pl.pallas_call(
            functools.partial(pack_kernel, share=share),
            out_shape=jax.ShapeDtypeStruct((tokens + rope_rows, columns), BF16),
            in_specs=[HBM, HBM],
            out_specs=VMEM,
            scratch_shapes=[
                pltpu.VMEM((share, ROPE), BF16),
                pltpu.SemaphoreType.DMA((2,)),
            ],
            compiler_params=pltpu.CompilerParams(vmem_limit_bytes=2 * MIB),
            name="pack",
        )(kv_latent, key_rope)

        stack = piece[None]
        for number, mask in enumerate(masks[:-1]):
            received = exchange(stack, mask)
            if number == len(masks) - 4:
                received, nope, top = lax.optimization_barrier((received, *load(stack)))
            elif number == len(masks) - 3:
                received, query_cos, query_sin, cosine, sine, bias, rope, bottom = (
                    lax.optimization_barrier((received, *tables(stack)))
                )
            elif number == len(masks) - 2:
                break
            stack = jnp.concatenate([stack, received], 0)
        sibling = exchange(stack, masks[-1])
        _, *arrays = lax.optimization_barrier(
            (stack, query_cos, query_sin, nope, rope, top, bottom)
        )
        received, sibling, query = lax.optimization_barrier((received, sibling, absorb(*arrays)))
        stack = jnp.concatenate([stack, received, sibling, exchange(received, masks[-1])], 0)

        keys = ctx_size * tokens
        scratch = [
            pltpu.VMEM((keys, latent_width + LANES), BF16),
            pltpu.VMEM((tokens, heads * VALUE_DIM), BF16),
            pltpu.SemaphoreType.DMA((len(groups),)),
        ]
        if blocks > 1:
            scratch += [
                pltpu.VMEM((max(groups) * tokens, LANES), F32),
                pltpu.VMEM((max(groups) * tokens, LANES), F32),
                pltpu.VMEM((max(groups) * tokens, latent_width), F32),
            ]
        return pl.pallas_call(
            functools.partial(
                attend_kernel,
                ctx_columns=ctx_columns,
                head_columns=head_columns,
                share=share,
                groups=groups,
                ahead=2,
            ),
            out_shape=jax.ShapeDtypeStruct((tokens, heads * VALUE_DIM), BF16),
            in_specs=[VMEM] * 7,
            out_specs=HBM,
            scratch_shapes=scratch,
            compiler_params=pltpu.CompilerParams(vmem_limit_bytes=24 * MIB),
            name="attend",
        )(stack, query, cosine, sine, bias, latent_gain.reshape(1, latent_width), w_value)

    return per_device


def solution(mesh):
    sizes = mesh.shape["ctx"], mesh.shape["head"]
    return jax.shard_map(
        make_per_device(sizes, exchange_masks(mesh)),
        mesh=mesh,
        in_specs=(
            P(("group", "ctx"), "head"),
            P(("group", "ctx"), "head"),
            P(("group", "ctx"), "head"),
            P(("group", "ctx"), None),
            P(),
            P(None, "head"),
            P(None, "head"),
            P("group"),
        ),
        out_specs=P(("group", "ctx"), "head"),
        check_vma=False,
    )
```

```python
import functools
import math

import jax
import jax.numpy as jnp
from jax import lax
from jax.experimental import pallas as pl
from jax.experimental.pallas import tpu as pltpu
from jax.sharding import PartitionSpec as P

ROPE = 64
NOPE = 128
VALUE_DIM = 128
LANES = 128

EPSILON = 1e-06
NEGATIVE = -1e30
SCALE = math.log2(math.e) / math.sqrt(NOPE + ROPE)


BF16 = jnp.bfloat16
F32 = jnp.float32
VMEM = pl.BlockSpec(memory_space=pltpu.VMEM)
ANY = pl.BlockSpec(memory_space=pl.ANY)
HBM = pl.BlockSpec(memory_space=pltpu.MemorySpace.HBM)
MIB = 1 << 20


def same_chip(one, other):
    place = getattr(one, "coords", None)
    return place is not None and one.id != other.id and place == getattr(other, "coords", None)


def exchange_masks(mesh):
    sizes = mesh.shape["ctx"], mesh.shape["head"]
    devices = mesh.devices.transpose([mesh.axis_names.index(n) for n in ("group", "ctx", "head")])
    core = None
    for axis, bit in ((1, (1, 0)), (2, (0, 1))):
        if sizes[axis - 1] > 1 and same_chip(devices[0, 0, 0], devices[(0, *bit)]):
            core = bit
    masks = []
    for axis, size in enumerate(sizes):
        while size > 1:
            size //= 2
            mask = (size, 0) if axis == 0 else (0, size)
            if mask != core:
                masks.append(mask)
    if core is not None:
        masks = [(c ^ core[0], h ^ core[1]) for c, h in masks] + [core]
    return masks


def stack_columns(masks, sizes):
    index_of = {(0, 0): 0}
    for bit, (c, h) in enumerate(masks):
        index_of |= {(i ^ c, j ^ h): at ^ (1 << bit) for (i, j), at in index_of.items()}
    ctx_bits = range(sizes[0].bit_length() - 1)
    head_bits = range(sizes[1].bit_length() - 1)
    return [index_of[1 << b, 0] for b in ctx_bits], [index_of[0, 1 << b] for b in head_bits]


def combine(offset, columns):
    index = 0
    for bit, column in enumerate(columns):
        index = index ^ (((offset >> bit) & 1) * column)
    return index


def swap_halves(values):
    half = ROPE // 2
    lane = lax.broadcasted_iota(jnp.int32, values.shape, 1)
    width = values.shape[1]
    return jnp.where(
        lane % ROPE < half, pltpu.roll(values, width - half, 1), pltpu.roll(values, half, 1)
    )


def rotation_tables(place):
    half = ROPE // 2
    lane = lax.broadcasted_iota(jnp.int32, place.shape, 1)
    frequency = jnp.exp(-math.log(10000.0) * (lane % half).astype(F32) / half)
    angle = place.astype(F32) * frequency
    sine = jnp.sin(angle)
    return jnp.cos(angle), jnp.where(lane % ROPE < half, -sine, sine)


def places_of(token, early, late, block_rows):
    return jnp.where(token < block_rows, early, late) * block_rows + token % block_rows


def pack_kernel(latent_hbm, rope_hbm, piece_ref, rope_ref, sems, *, share):
    tokens = latent_hbm.shape[0]
    fold = LANES // ROPE
    rows = share // fold
    first = pl.multiple_of(lax.axis_index("head") * share, share)
    latent_copy = pltpu.make_async_copy(latent_hbm, piece_ref.at[pl.ds(0, tokens)], sems.at[0])
    rope_copy = pltpu.make_async_copy(rope_hbm.at[pl.ds(first, share)], rope_ref, sems.at[1])
    latent_copy.start()
    rope_copy.start()
    rope_copy.wait()
    mine = rope_ref[...].astype(F32)
    parts = [mine[f * rows : (f + 1) * rows] for f in range(fold)]
    piece_ref[tokens:] = jnp.concatenate(parts, 1).astype(BF16)
    latent_copy.wait()


def absorb_kernel(
    cos_ref, sin_ref, nope_ref, rope_ref, top_ref, w_key_hbm, query_ref, bottom_ref, sems
):
    tokens = nope_ref.shape[0]
    part = top_ref.shape[0]
    heads = top_ref.shape[1] // NOPE
    fold = LANES // ROPE
    bottom_copy = pltpu.make_async_copy(w_key_hbm.at[pl.ds(part, part)], bottom_ref, sems.at[0])
    bottom_copy.start()

    def absorb(w_key_ref, first):
        for head in range(heads):
            columns = slice(head * NOPE, (head + 1) * NOPE)
            absorbed = lax.dot_general(
                nope_ref[:, columns],
                w_key_ref[:, columns],
                (((1,), (1,)), ((), ())),
                preferred_element_type=F32,
            )
            query_ref[head * tokens : (head + 1) * tokens, first : first + part] = (
                absorbed.astype(BF16)
            )

    absorb(top_ref, 0)
    lane = lax.broadcasted_iota(jnp.int32, (tokens, LANES), 1)
    for pair in range(heads // fold):
        values = rope_ref[:, pair * LANES : (pair + 1) * LANES].astype(F32)
        rotated = values * cos_ref[...] + swap_halves(values) * sin_ref[...]
        for f in range(fold):
            head = pair * fold + f
            kept = jnp.where(lane // ROPE == f, rotated, 0.0)
            query_ref[head * tokens : (head + 1) * tokens, 2 * part :] = kept.astype(BF16)
    bottom_copy.wait()
    absorb(bottom_ref, part)


def table_kernel(
    _,
    order_hbm,
    nope_hbm,
    rope_hbm,
    w_key_hbm,
    query_cos_ref,
    query_sin_ref,
    cos_ref,
    sin_ref,
    bias_ref,
    nope_ref,
    rope_ref,
    top_ref,
    order_ref,
    sems,
    *,
    share,
):
    tokens = query_cos_ref.shape[0]
    fold = LANES // ROPE
    rows = share // fold
    block_rows = tokens // 2
    ctx_count, table_rows, _ = cos_ref.shape
    order_copy = pltpu.make_async_copy(order_hbm, order_ref, sems.at[0])
    copies = [
        pltpu.make_async_copy(w_key_hbm.at[pl.ds(0, top_ref.shape[0])], top_ref, sems.at[1]),
        pltpu.make_async_copy(nope_hbm, nope_ref, sems.at[2]),
        pltpu.make_async_copy(rope_hbm, rope_ref, sems.at[3]),
    ]
    order_copy.start()
    for copy in copies:
        copy.start()
    order_copy.wait()
    ctx_here = lax.axis_index("ctx")
    early = order_ref[2 * ctx_here]
    late = order_ref[2 * ctx_here + 1]
    query_token = lax.broadcasted_iota(jnp.int32, (tokens, LANES), 0)
    query_cos_ref[...], query_sin_ref[...] = rotation_tables(
        places_of(query_token, early, late, block_rows)
    )
    row = lax.broadcasted_iota(jnp.int32, (table_rows, LANES), 0)
    lane = lax.broadcasted_iota(jnp.int32, (table_rows, LANES), 1)
    token = (row // rows) * share + (lane // ROPE) * rows + row % rows
    blocks, _, block = bias_ref.shape
    chunks_per_block = block // tokens
    query_token = lax.broadcasted_iota(jnp.int32, (tokens, block), 0)
    query_place = places_of(query_token, early, late, block_rows)
    key_lane = lax.broadcasted_iota(jnp.int32, (tokens, block), 1)

    def one(b, unused):
        key_place = None
        for i in range(chunks_per_block):
            c = b * chunks_per_block + i
            source = ctx_here ^ c
            early = order_ref[2 * source]
            late = order_ref[2 * source + 1]
            cos_ref[c], sin_ref[c] = rotation_tables(places_of(token, early, late, block_rows))
            place = places_of(key_lane % tokens, early, late, block_rows)
            key_place = place if i == 0 else jnp.where(key_lane < i * tokens, key_place, place)
        bias_ref[b] = jnp.where(key_place <= query_place, 0.0, NEGATIVE)
        return unused

    if blocks == 1:
        one(0, 0)
    else:
        lax.fori_loop(0, blocks, one, 0)
    for copy in copies:
        copy.wait()


def attend_kernel(
    stack_ref,
    query_ref,
    cos_ref,
    sin_ref,
    bias_ref,
    gain_ref,
    w_value_ref,
    out_hbm,
    key_ref,
    out_ref,
    sems,
    *run_refs,
    ctx_columns,
    head_columns,
    share,
    groups,
    ahead,
):
    tokens = bias_ref.shape[1]
    columns = stack_ref.shape[2]
    latent_width = w_value_ref.shape[0]
    heads = w_value_ref.shape[1] // VALUE_DIM
    ctx_count = cos_ref.shape[0]
    head_count = latent_width // columns
    fold = LANES // ROPE
    rope_rows = share // fold
    starts = [sum(groups[:g]) for g in range(len(groups))]
    head_here = lax.axis_index("head")
    places = [combine(head_here ^ h, head_columns) for h in range(head_count)]
    lane = lax.broadcasted_iota(jnp.int32, (rope_rows, LANES), 1)

    def one_chunk(c, unused):
        first = c * tokens
        if not isinstance(c, int):
            first = pl.multiple_of(first, tokens)
        rows = pl.ds(first, tokens)
        here = combine(c, ctx_columns)
        parts = [stack_ref[p ^ here, :tokens, :].astype(F32) for p in places]
        square = functools.reduce(jnp.add, [x * x for x in parts])
        mean = jnp.sum(square, axis=1, keepdims=True) * (1.0 / latent_width)
        factor = lax.rsqrt(mean + EPSILON)
        for h, x in enumerate(parts):
            gain = gain_ref[:, h * columns : (h + 1) * columns]
            key_ref[rows, h * columns : (h + 1) * columns] = (x * factor * gain).astype(BF16)
        pieces = []
        for h, p in enumerate(places):
            values = stack_ref[p ^ here, tokens:, :].astype(F32)
            table = slice(h * rope_rows, (h + 1) * rope_rows)
            values = values * cos_ref[c, table] + swap_halves(values) * sin_ref[c, table]
            turned = pltpu.roll(values, ROPE, 1)
            pieces.append(jnp.where(lane < ROPE, values, turned))
            pieces.append(jnp.where(lane < ROPE, turned, values))
        key_ref[rows, latent_width:] = jnp.concatenate(pieces, 0).astype(BF16)
        return unused

    if ctx_count <= 8:
        for c in range(ctx_count):
            one_chunk(c, 0)
    else:
        lax.fori_loop(0, ctx_count, one_chunk, 0)

    def scores_of(g, keys):
        first = starts[g] * tokens
        query = query_ref[first : first + groups[g] * tokens, :]
        return lax.dot_general(query, keys, (((1,), (1,)), ((), ())), preferred_element_type=F32)

    def masked(scores, b):
        return scores.reshape(-1, tokens, scores.shape[1]) * SCALE + bias_ref[b][None]

    def out_copy(g):
        where = pl.ds(starts[g] * VALUE_DIM, groups[g] * VALUE_DIM)
        return pltpu.make_async_copy(out_ref.at[:, where], out_hbm.at[:, where], sems.at[g])

    def finish(g, mixed, total):
        mixed = (mixed * (1.0 / total)).astype(BF16)
        for i in range(groups[g]):
            head = starts[g] + i
            where = slice(head * VALUE_DIM, (head + 1) * VALUE_DIM)
            out_ref[:, where] = jnp.dot(
                mixed[i * tokens : (i + 1) * tokens],
                w_value_ref[:, where],
                preferred_element_type=F32,
            ).astype(BF16)
        out_copy(g).start()

    if bias_ref.shape[0] == 1:
        scores = [scores_of(g, key_ref[...]) for g in range(min(ahead, len(groups)))]
        for g in range(len(groups)):
            now = masked(scores[g], 0)
            if g + ahead < len(groups):
                scores.append(scores_of(g + ahead, key_ref[...]))
            exps = jnp.exp2(now - jnp.max(now, axis=2, keepdims=True))
            total = jnp.sum(exps, axis=2, keepdims=True).reshape(-1, 1)
            mixed = jnp.dot(
                exps.reshape(-1, exps.shape[2]).astype(BF16),
                key_ref[:, :latent_width],
                preferred_element_type=F32,
            )
            finish(g, mixed, total)
    else:
        max_ref, total_ref, mixed_ref = run_refs
        block = bias_ref.shape[2]
        for g, group in enumerate(groups):
            height = group * tokens
            rows = slice(0, height)
            max_ref[rows] = jnp.full((height, LANES), NEGATIVE, F32)
            total_ref[rows] = jnp.zeros((height, LANES), F32)
            mixed_ref[rows] = jnp.zeros((height, latent_width), F32)

            def one_block(b, unused):
                keys = key_ref[pl.ds(pl.multiple_of(b * block, block), block), :]
                now = masked(scores_of(g, keys), b)
                old = max_ref[rows, :1].reshape(group, tokens, 1)
                new = jnp.maximum(old, jnp.max(now, axis=2, keepdims=True))
                exps = jnp.where(bias_ref[b][None] < 0.0, 0.0, jnp.exp2(now - new))
                shrink = jnp.exp2(old - new).reshape(height, 1)
                total = jnp.sum(exps, axis=2, keepdims=True).reshape(height, 1)
                max_ref[rows] = jnp.broadcast_to(new.reshape(height, 1), (height, LANES))
                total_ref[rows] = total_ref[rows] * shrink + total
                mixed_ref[rows] = mixed_ref[rows] * shrink + jnp.dot(
                    exps.reshape(height, block).astype(BF16),
                    keys[:, :latent_width],
                    preferred_element_type=F32,
                )
                return unused

            lax.fori_loop(0, bias_ref.shape[0], one_block, 0)
            finish(g, mixed_ref[rows], total_ref[rows, :1])
    for g in range(len(groups)):
        out_copy(g).wait()


def head_groups(heads):
    if heads < 3:
        return [heads]
    return [heads // 3, heads - 2 * (heads // 3), heads // 3]


def make_per_device(sizes, masks):
    ctx_size, head_size = sizes
    ctx_columns, head_columns = stack_columns(masks, sizes)
    everyone = [(c, h) for c in range(ctx_size) for h in range(head_size)]

    def exchange(stack, mask):
        pairs = [
            (c * head_size + h, (c ^ mask[0]) * head_size + (h ^ mask[1])) for c, h in everyone
        ]
        return lax.ppermute(stack, ("ctx", "head"), pairs)

    def per_device(
        query_nope, query_rope, kv_latent, key_rope, latent_gain, w_key, w_value, block_order
    ):
        tokens, columns = kv_latent.shape
        heads = w_key.shape[1] // NOPE
        latent_width = w_key.shape[0]
        query_nope, query_rope, kv_latent, key_rope, w_key, block_order = (
            pltpu.with_memory_space_constraint(x, pltpu.MemorySpace.HBM)
            for x in (query_nope, query_rope, kv_latent, key_rope, w_key, block_order)
        )
        share = tokens // head_size
        rope_rows = share * ROPE // LANES
        groups = head_groups(heads)
        chunks_per_block = min(ctx_size, max(1, 256 // tokens))
        blocks = ctx_size // chunks_per_block

        half_key = jax.ShapeDtypeStruct((latent_width // 2, heads * NOPE), BF16)

        def tables(after):
            query_table = jax.ShapeDtypeStruct((tokens, LANES), F32)
            table = jax.ShapeDtypeStruct((ctx_size, head_size * rope_rows, LANES), F32)
            bias = jax.ShapeDtypeStruct((blocks, tokens, chunks_per_block * tokens), F32)
            nope = jax.ShapeDtypeStruct((tokens, heads * NOPE), BF16)
            rope = jax.ShapeDtypeStruct((tokens, heads * ROPE), BF16)
            return pl.pallas_call(
                functools.partial(table_kernel, share=share),
                out_shape=(query_table, query_table, table, table, bias, nope, rope, half_key),
                in_specs=[ANY] + [HBM] * 4,
                out_specs=(VMEM,) * 8,
                scratch_shapes=[
                    pltpu.SMEM(block_order.shape, jnp.int32),
                    pltpu.SemaphoreType.DMA((4,)),
                ],
                compiler_params=pltpu.CompilerParams(vmem_limit_bytes=8 * MIB),
                name="tables",
            )(after, block_order, query_nope, query_rope, w_key)

        def absorb(*arrays):
            return pl.pallas_call(
                absorb_kernel,
                out_shape=jax.ShapeDtypeStruct((heads * tokens, latent_width + LANES), BF16),
                in_specs=[VMEM] * 5 + [HBM],
                out_specs=VMEM,
                scratch_shapes=[
                    pltpu.VMEM(half_key.shape, BF16),
                    pltpu.SemaphoreType.DMA((1,)),
                ],
                compiler_params=pltpu.CompilerParams(vmem_limit_bytes=8 * MIB),
                name="absorb",
            )(*arrays, w_key)

        piece = pl.pallas_call(
            functools.partial(pack_kernel, share=share),
            out_shape=jax.ShapeDtypeStruct((tokens + rope_rows, columns), BF16),
            in_specs=[HBM, HBM],
            out_specs=VMEM,
            scratch_shapes=[
                pltpu.VMEM((share, ROPE), BF16),
                pltpu.SemaphoreType.DMA((2,)),
            ],
            compiler_params=pltpu.CompilerParams(vmem_limit_bytes=2 * MIB),
            name="pack",
        )(kv_latent, key_rope)

        stack = piece[None]
        for number, mask in enumerate(masks[:-2]):
            received = exchange(stack, mask)
            if number == len(masks) - 4:
                received, query_cos, query_sin, cosine, sine, bias, nope, rope, top = (
                    lax.optimization_barrier((received, *tables(stack)))
                )
            elif number == len(masks) - 3:
                early = exchange(stack, masks[-2])
                fresh = received
            stack = jnp.concatenate([stack, received], 0)
        received = exchange(fresh, masks[-2])
        _, *arrays = lax.optimization_barrier((fresh, query_cos, query_sin, nope, rope, top))
        received, early, query = lax.optimization_barrier((received, early, absorb(*arrays)))
        stack = jnp.concatenate([stack, early, received], 0)
        stack = jnp.concatenate([stack, exchange(stack, masks[-1])], 0)

        keys = ctx_size * tokens
        scratch = [
            pltpu.VMEM((keys, latent_width + LANES), BF16),
            pltpu.VMEM((tokens, heads * VALUE_DIM), BF16),
            pltpu.SemaphoreType.DMA((len(groups),)),
        ]
        if blocks > 1:
            scratch += [
                pltpu.VMEM((max(groups) * tokens, LANES), F32),
                pltpu.VMEM((max(groups) * tokens, LANES), F32),
                pltpu.VMEM((max(groups) * tokens, latent_width), F32),
            ]
        return pl.pallas_call(
            functools.partial(
                attend_kernel,
                ctx_columns=ctx_columns,
                head_columns=head_columns,
                share=share,
                groups=groups,
                ahead=2,
            ),
            out_shape=jax.ShapeDtypeStruct((tokens, heads * VALUE_DIM), BF16),
            in_specs=[VMEM] * 7,
            out_specs=HBM,
            scratch_shapes=scratch,
            compiler_params=pltpu.CompilerParams(vmem_limit_bytes=24 * MIB),
            name="attend",
        )(stack, query, cosine, sine, bias, latent_gain.reshape(1, latent_width), w_value)

    return per_device


def solution(mesh):
    sizes = mesh.shape["ctx"], mesh.shape["head"]
    return jax.shard_map(
        make_per_device(sizes, exchange_masks(mesh)),
        mesh=mesh,
        in_specs=(
            P(("group", "ctx"), "head"),
            P(("group", "ctx"), "head"),
            P(("group", "ctx"), "head"),
            P(("group", "ctx"), None),
            P(),
            P(None, "head"),
            P(None, "head"),
            P("group"),
        ),
        out_specs=P(("group", "ctx"), "head"),
        check_vma=False,
    )
```

```python
import functools
import math

import jax
import jax.numpy as jnp
from jax import lax
from jax.experimental import pallas as pl
from jax.experimental.pallas import tpu as pltpu
from jax.sharding import PartitionSpec as P

ROPE = 64
NOPE = 128
VALUE_DIM = 128
LANES = 128

EPSILON = 1e-06
NEGATIVE = -1e30
SCALE = math.log2(math.e) / math.sqrt(NOPE + ROPE)


BF16 = jnp.bfloat16
F32 = jnp.float32
VMEM = pl.BlockSpec(memory_space=pltpu.VMEM)
ANY = pl.BlockSpec(memory_space=pl.ANY)
HBM = pl.BlockSpec(memory_space=pltpu.MemorySpace.HBM)
MIB = 1 << 20


def same_chip(one, other):
    place = getattr(one, "coords", None)
    return place is not None and one.id != other.id and place == getattr(other, "coords", None)


def exchange_masks(mesh):
    sizes = mesh.shape["ctx"], mesh.shape["head"]
    devices = mesh.devices.transpose([mesh.axis_names.index(n) for n in ("group", "ctx", "head")])
    core = None
    for axis, bit in ((1, (1, 0)), (2, (0, 1))):
        if sizes[axis - 1] > 1 and same_chip(devices[0, 0, 0], devices[(0, *bit)]):
            core = bit
    masks = []
    for axis, size in enumerate(sizes):
        while size > 1:
            size //= 2
            mask = (size, 0) if axis == 0 else (0, size)
            if mask != core:
                masks.append(mask)
    if core is not None:
        masks = [(c ^ core[0], h ^ core[1]) for c, h in masks] + [core]
    return masks


def stack_columns(masks, sizes):
    index_of = {(0, 0): 0}
    for bit, (c, h) in enumerate(masks):
        index_of |= {(i ^ c, j ^ h): at ^ (1 << bit) for (i, j), at in index_of.items()}
    ctx_bits = range(sizes[0].bit_length() - 1)
    head_bits = range(sizes[1].bit_length() - 1)
    return [index_of[1 << b, 0] for b in ctx_bits], [index_of[0, 1 << b] for b in head_bits]


def combine(offset, columns):
    index = 0
    for bit, column in enumerate(columns):
        index = index ^ (((offset >> bit) & 1) * column)
    return index


def swap_halves(values):
    half = ROPE // 2
    lane = lax.broadcasted_iota(jnp.int32, values.shape, 1)
    width = values.shape[1]
    return jnp.where(
        lane % ROPE < half, pltpu.roll(values, width - half, 1), pltpu.roll(values, half, 1)
    )


def rotation_tables(place):
    half = ROPE // 2
    lane = lax.broadcasted_iota(jnp.int32, place.shape, 1)
    frequency = jnp.exp(-math.log(10000.0) * (lane % half).astype(F32) / half)
    angle = place.astype(F32) * frequency
    sine = jnp.sin(angle)
    return jnp.cos(angle), jnp.where(lane % ROPE < half, -sine, sine)


def places_of(token, early, late, block_rows):
    return jnp.where(token < block_rows, early, late) * block_rows + token % block_rows


def pack_kernel(latent_hbm, rope_hbm, piece_ref, rope_ref, sems, *, share):
    tokens = latent_hbm.shape[0]
    fold = LANES // ROPE
    rows = share // fold
    first = pl.multiple_of(lax.axis_index("head") * share, share)
    latent_copy = pltpu.make_async_copy(latent_hbm, piece_ref.at[pl.ds(0, tokens)], sems.at[0])
    rope_copy = pltpu.make_async_copy(rope_hbm.at[pl.ds(first, share)], rope_ref, sems.at[1])
    latent_copy.start()
    rope_copy.start()
    rope_copy.wait()
    mine = rope_ref[...].astype(F32)
    parts = [mine[f * rows : (f + 1) * rows] for f in range(fold)]
    piece_ref[tokens:] = jnp.concatenate(parts, 1).astype(BF16)
    latent_copy.wait()


def absorb_into(query_ref, nope_ref, w_key_ref):
    tokens = nope_ref.shape[0]
    width = w_key_ref.shape[0]
    for head in range(w_key_ref.shape[1] // NOPE):
        columns = slice(head * NOPE, (head + 1) * NOPE)
        absorbed = lax.dot_general(
            nope_ref[:, columns],
            w_key_ref[:, columns],
            (((1,), (1,)), ((), ())),
            preferred_element_type=F32,
        )
        query_ref[head * tokens : (head + 1) * tokens, :width] = absorbed.astype(BF16)


def absorb_kernel(
    cos_ref, sin_ref, nope_ref, rope_ref, top_ref, w_key_hbm, query_ref, bottom_ref, sems
):
    tokens = nope_ref.shape[0]
    part = top_ref.shape[0]
    heads = top_ref.shape[1] // NOPE
    fold = LANES // ROPE
    rest = bottom_ref.shape[0]
    bottom_copy = pltpu.make_async_copy(w_key_hbm.at[pl.ds(part, rest)], bottom_ref, sems.at[0])
    bottom_copy.start()
    absorb_into(query_ref, nope_ref, top_ref)
    lane = lax.broadcasted_iota(jnp.int32, (tokens, LANES), 1)
    for pair in range(heads // fold):
        values = rope_ref[:, pair * LANES : (pair + 1) * LANES].astype(F32)
        rotated = values * cos_ref[...] + swap_halves(values) * sin_ref[...]
        for f in range(fold):
            head = pair * fold + f
            kept = jnp.where(lane // ROPE == f, rotated, 0.0)
            query_ref[head * tokens : (head + 1) * tokens, part:] = kept.astype(BF16)
    bottom_copy.wait()


def absorb_rest_kernel(_, nope_ref, bottom_ref, query_ref):
    absorb_into(query_ref, nope_ref, bottom_ref)


def table_kernel(
    _,
    order_hbm,
    nope_hbm,
    rope_hbm,
    w_key_hbm,
    query_cos_ref,
    query_sin_ref,
    cos_ref,
    sin_ref,
    bias_ref,
    nope_ref,
    rope_ref,
    top_ref,
    order_ref,
    sems,
    *,
    share,
):
    tokens = query_cos_ref.shape[0]
    fold = LANES // ROPE
    rows = share // fold
    block_rows = tokens // 2
    ctx_count, table_rows, _ = cos_ref.shape
    order_copy = pltpu.make_async_copy(order_hbm, order_ref, sems.at[0])
    copies = [
        pltpu.make_async_copy(w_key_hbm.at[pl.ds(0, top_ref.shape[0])], top_ref, sems.at[1]),
        pltpu.make_async_copy(nope_hbm, nope_ref, sems.at[2]),
        pltpu.make_async_copy(rope_hbm, rope_ref, sems.at[3]),
    ]
    order_copy.start()
    for copy in copies:
        copy.start()
    order_copy.wait()
    ctx_here = lax.axis_index("ctx")
    early = order_ref[2 * ctx_here]
    late = order_ref[2 * ctx_here + 1]
    query_token = lax.broadcasted_iota(jnp.int32, (tokens, LANES), 0)
    query_cos_ref[...], query_sin_ref[...] = rotation_tables(
        places_of(query_token, early, late, block_rows)
    )
    row = lax.broadcasted_iota(jnp.int32, (table_rows, LANES), 0)
    lane = lax.broadcasted_iota(jnp.int32, (table_rows, LANES), 1)
    token = (row // rows) * share + (lane // ROPE) * rows + row % rows
    blocks, _, block = bias_ref.shape
    chunks_per_block = block // tokens
    query_token = lax.broadcasted_iota(jnp.int32, (tokens, block), 0)
    query_place = places_of(query_token, early, late, block_rows)
    key_lane = lax.broadcasted_iota(jnp.int32, (tokens, block), 1)

    def one(b, unused):
        key_place = None
        for i in range(chunks_per_block):
            c = b * chunks_per_block + i
            source = ctx_here ^ c
            early = order_ref[2 * source]
            late = order_ref[2 * source + 1]
            cos_ref[c], sin_ref[c] = rotation_tables(places_of(token, early, late, block_rows))
            place = places_of(key_lane % tokens, early, late, block_rows)
            key_place = place if i == 0 else jnp.where(key_lane < i * tokens, key_place, place)
        bias_ref[b] = jnp.where(key_place <= query_place, 0.0, NEGATIVE)
        return unused

    if blocks == 1:
        one(0, 0)
    else:
        lax.fori_loop(0, blocks, one, 0)
    for copy in copies:
        copy.wait()


def attend_kernel(
    stack_ref,
    query_ref,
    rest_ref,
    cos_ref,
    sin_ref,
    bias_ref,
    gain_ref,
    w_value_ref,
    out_hbm,
    key_ref,
    out_ref,
    sems,
    *run_refs,
    ctx_columns,
    head_columns,
    share,
    groups,
    ahead,
):
    tokens = bias_ref.shape[1]
    columns = stack_ref.shape[2]
    latent_width = w_value_ref.shape[0]
    heads = w_value_ref.shape[1] // VALUE_DIM
    ctx_count = cos_ref.shape[0]
    head_count = latent_width // columns
    fold = LANES // ROPE
    rope_rows = share // fold
    starts = [sum(groups[:g]) for g in range(len(groups))]
    head_here = lax.axis_index("head")
    places = [combine(head_here ^ h, head_columns) for h in range(head_count)]
    lane = lax.broadcasted_iota(jnp.int32, (rope_rows, LANES), 1)

    def one_chunk(c, unused):
        first = c * tokens
        if not isinstance(c, int):
            first = pl.multiple_of(first, tokens)
        rows = pl.ds(first, tokens)
        here = combine(c, ctx_columns)
        parts = [stack_ref[p ^ here, :tokens, :].astype(F32) for p in places]
        square = functools.reduce(jnp.add, [x * x for x in parts])
        mean = jnp.sum(square, axis=1, keepdims=True) * (1.0 / latent_width)
        factor = lax.rsqrt(mean + EPSILON)
        for h, x in enumerate(parts):
            gain = gain_ref[:, h * columns : (h + 1) * columns]
            key_ref[rows, h * columns : (h + 1) * columns] = (x * factor * gain).astype(BF16)
        pieces = []
        for h, p in enumerate(places):
            values = stack_ref[p ^ here, tokens:, :].astype(F32)
            table = slice(h * rope_rows, (h + 1) * rope_rows)
            values = values * cos_ref[c, table] + swap_halves(values) * sin_ref[c, table]
            turned = pltpu.roll(values, ROPE, 1)
            pieces.append(jnp.where(lane < ROPE, values, turned))
            pieces.append(jnp.where(lane < ROPE, turned, values))
        key_ref[rows, latent_width:] = jnp.concatenate(pieces, 0).astype(BF16)
        return unused

    if ctx_count <= 8:
        for c in range(ctx_count):
            one_chunk(c, 0)
    else:
        lax.fori_loop(0, ctx_count, one_chunk, 0)

    def scores_of(g, keys):
        first = starts[g] * tokens
        rows = slice(first, first + groups[g] * tokens)
        part = latent_width - rest_ref.shape[1]
        query = jnp.concatenate(
            [query_ref[rows, :part], rest_ref[rows, :], query_ref[rows, part:]], 1
        )
        return lax.dot_general(query, keys, (((1,), (1,)), ((), ())), preferred_element_type=F32)

    def masked(scores, b):
        return scores.reshape(-1, tokens, scores.shape[1]) * SCALE + bias_ref[b][None]

    def out_copy(g):
        where = pl.ds(starts[g] * VALUE_DIM, groups[g] * VALUE_DIM)
        return pltpu.make_async_copy(out_ref.at[:, where], out_hbm.at[:, where], sems.at[g])

    def finish(g, mixed, total):
        mixed = (mixed * (1.0 / total)).astype(BF16)
        for i in range(groups[g]):
            head = starts[g] + i
            where = slice(head * VALUE_DIM, (head + 1) * VALUE_DIM)
            out_ref[:, where] = jnp.dot(
                mixed[i * tokens : (i + 1) * tokens],
                w_value_ref[:, where],
                preferred_element_type=F32,
            ).astype(BF16)
        out_copy(g).start()

    if bias_ref.shape[0] == 1:
        scores = [scores_of(g, key_ref[...]) for g in range(min(ahead, len(groups)))]
        for g in range(len(groups)):
            now = masked(scores[g], 0)
            if g + ahead < len(groups):
                scores.append(scores_of(g + ahead, key_ref[...]))
            exps = jnp.exp2(now - jnp.max(now, axis=2, keepdims=True))
            total = jnp.sum(exps, axis=2, keepdims=True).reshape(-1, 1)
            mixed = jnp.dot(
                exps.reshape(-1, exps.shape[2]).astype(BF16),
                key_ref[:, :latent_width],
                preferred_element_type=F32,
            )
            finish(g, mixed, total)
    else:
        max_ref, total_ref, mixed_ref = run_refs
        block = bias_ref.shape[2]
        for g, group in enumerate(groups):
            height = group * tokens
            rows = slice(0, height)
            max_ref[rows] = jnp.full((height, LANES), NEGATIVE, F32)
            total_ref[rows] = jnp.zeros((height, LANES), F32)
            mixed_ref[rows] = jnp.zeros((height, latent_width), F32)

            def one_block(b, unused):
                keys = key_ref[pl.ds(pl.multiple_of(b * block, block), block), :]
                now = masked(scores_of(g, keys), b)
                old = max_ref[rows, :1].reshape(group, tokens, 1)
                new = jnp.maximum(old, jnp.max(now, axis=2, keepdims=True))
                exps = jnp.where(bias_ref[b][None] < 0.0, 0.0, jnp.exp2(now - new))
                shrink = jnp.exp2(old - new).reshape(height, 1)
                total = jnp.sum(exps, axis=2, keepdims=True).reshape(height, 1)
                max_ref[rows] = jnp.broadcast_to(new.reshape(height, 1), (height, LANES))
                total_ref[rows] = total_ref[rows] * shrink + total
                mixed_ref[rows] = mixed_ref[rows] * shrink + jnp.dot(
                    exps.reshape(height, block).astype(BF16),
                    keys[:, :latent_width],
                    preferred_element_type=F32,
                )
                return unused

            lax.fori_loop(0, bias_ref.shape[0], one_block, 0)
            finish(g, mixed_ref[rows], total_ref[rows, :1])
    for g in range(len(groups)):
        out_copy(g).wait()


def head_groups(heads):
    if heads < 3:
        return [heads]
    return [heads // 3, heads - 2 * (heads // 3), heads // 3]


def make_per_device(sizes, masks):
    ctx_size, head_size = sizes
    ctx_columns, head_columns = stack_columns(masks, sizes)
    everyone = [(c, h) for c in range(ctx_size) for h in range(head_size)]

    def exchange(stack, mask):
        pairs = [
            (c * head_size + h, (c ^ mask[0]) * head_size + (h ^ mask[1])) for c, h in everyone
        ]
        return lax.ppermute(stack, ("ctx", "head"), pairs)

    def per_device(
        query_nope, query_rope, kv_latent, key_rope, latent_gain, w_key, w_value, block_order
    ):
        tokens, columns = kv_latent.shape
        heads = w_key.shape[1] // NOPE
        latent_width = w_key.shape[0]
        query_nope, query_rope, kv_latent, key_rope, w_key, block_order = (
            pltpu.with_memory_space_constraint(x, pltpu.MemorySpace.HBM)
            for x in (query_nope, query_rope, kv_latent, key_rope, w_key, block_order)
        )
        share = tokens // head_size
        rope_rows = share * ROPE // LANES
        groups = head_groups(heads)
        chunks_per_block = min(ctx_size, max(1, 256 // tokens))
        blocks = ctx_size // chunks_per_block

        half_key = jax.ShapeDtypeStruct((latent_width // 2, heads * NOPE), BF16)

        def tables(after):
            query_table = jax.ShapeDtypeStruct((tokens, LANES), F32)
            table = jax.ShapeDtypeStruct((ctx_size, head_size * rope_rows, LANES), F32)
            bias = jax.ShapeDtypeStruct((blocks, tokens, chunks_per_block * tokens), F32)
            nope = jax.ShapeDtypeStruct((tokens, heads * NOPE), BF16)
            rope = jax.ShapeDtypeStruct((tokens, heads * ROPE), BF16)
            return pl.pallas_call(
                functools.partial(table_kernel, share=share),
                out_shape=(query_table, query_table, table, table, bias, nope, rope, half_key),
                in_specs=[ANY] + [HBM] * 4,
                out_specs=(VMEM,) * 8,
                scratch_shapes=[
                    pltpu.SMEM(block_order.shape, jnp.int32),
                    pltpu.SemaphoreType.DMA((4,)),
                ],
                compiler_params=pltpu.CompilerParams(vmem_limit_bytes=8 * MIB),
                name="tables",
            )(after, block_order, query_nope, query_rope, w_key)

        def absorb(*arrays):
            return pl.pallas_call(
                absorb_kernel,
                out_shape=(
                    jax.ShapeDtypeStruct((heads * tokens, latent_width // 2 + LANES), BF16),
                    half_key,
                ),
                in_specs=[VMEM] * 5 + [HBM],
                out_specs=(VMEM, VMEM),
                scratch_shapes=[pltpu.SemaphoreType.DMA((1,))],
                compiler_params=pltpu.CompilerParams(vmem_limit_bytes=8 * MIB),
                name="absorb",
            )(*arrays, w_key)

        def absorb_rest(after, nope, bottom):
            return pl.pallas_call(
                absorb_rest_kernel,
                out_shape=jax.ShapeDtypeStruct((heads * tokens, latent_width // 2), BF16),
                in_specs=[ANY, VMEM, VMEM],
                out_specs=VMEM,
                compiler_params=pltpu.CompilerParams(vmem_limit_bytes=8 * MIB),
                name="absorb_rest",
            )(after, nope, bottom)

        piece = pl.pallas_call(
            functools.partial(pack_kernel, share=share),
            out_shape=jax.ShapeDtypeStruct((tokens + rope_rows, columns), BF16),
            in_specs=[HBM, HBM],
            out_specs=VMEM,
            scratch_shapes=[
                pltpu.VMEM((share, ROPE), BF16),
                pltpu.SemaphoreType.DMA((2,)),
            ],
            compiler_params=pltpu.CompilerParams(vmem_limit_bytes=2 * MIB),
            name="pack",
        )(kv_latent, key_rope)

        stack = piece[None]
        for number, mask in enumerate(masks[:-2]):
            received = exchange(stack, mask)
            if number == len(masks) - 4:
                received, query_cos, query_sin, cosine, sine, bias, nope, rope, top = (
                    lax.optimization_barrier((received, *tables(stack)))
                )
            elif number == len(masks) - 3:
                early = exchange(stack, masks[-2])
                fresh = received
            stack = jnp.concatenate([stack, received], 0)
        received = exchange(fresh, masks[-2])
        _, *arrays = lax.optimization_barrier((fresh, query_cos, query_sin, nope, rope, top))
        received, early, query, bottom = lax.optimization_barrier(
            (received, early, *absorb(*arrays))
        )
        stack = jnp.concatenate([stack, early, received], 0)
        received = exchange(stack, masks[-1])
        received, rest = lax.optimization_barrier((received, absorb_rest(stack, nope, bottom)))
        stack = jnp.concatenate([stack, received], 0)

        keys = ctx_size * tokens
        scratch = [
            pltpu.VMEM((keys, latent_width + LANES), BF16),
            pltpu.VMEM((tokens, heads * VALUE_DIM), BF16),
            pltpu.SemaphoreType.DMA((len(groups),)),
        ]
        if blocks > 1:
            scratch += [
                pltpu.VMEM((max(groups) * tokens, LANES), F32),
                pltpu.VMEM((max(groups) * tokens, LANES), F32),
                pltpu.VMEM((max(groups) * tokens, latent_width), F32),
            ]
        return pl.pallas_call(
            functools.partial(
                attend_kernel,
                ctx_columns=ctx_columns,
                head_columns=head_columns,
                share=share,
                groups=groups,
                ahead=2,
            ),
            out_shape=jax.ShapeDtypeStruct((tokens, heads * VALUE_DIM), BF16),
            in_specs=[VMEM] * 8,
            out_specs=HBM,
            scratch_shapes=scratch,
            compiler_params=pltpu.CompilerParams(vmem_limit_bytes=24 * MIB),
            name="attend",
        )(stack, query, rest, cosine, sine, bias, latent_gain.reshape(1, latent_width), w_value)

    return per_device


def solution(mesh):
    sizes = mesh.shape["ctx"], mesh.shape["head"]
    return jax.shard_map(
        make_per_device(sizes, exchange_masks(mesh)),
        mesh=mesh,
        in_specs=(
            P(("group", "ctx"), "head"),
            P(("group", "ctx"), "head"),
            P(("group", "ctx"), "head"),
            P(("group", "ctx"), None),
            P(),
            P(None, "head"),
            P(None, "head"),
            P("group"),
        ),
        out_specs=P(("group", "ctx"), "head"),
        check_vma=False,
    )
```

```python
import functools
import math

import jax
import jax.numpy as jnp
from jax import lax
from jax.experimental import pallas as pl
from jax.experimental.pallas import tpu as pltpu
from jax.sharding import PartitionSpec as P

ROPE = 64
NOPE = 128
VALUE_DIM = 128
LANES = 128

EPSILON = 1e-06
NEGATIVE = -1e30
SCALE = math.log2(math.e) / math.sqrt(NOPE + ROPE)


BF16 = jnp.bfloat16
F32 = jnp.float32
VMEM = pl.BlockSpec(memory_space=pltpu.VMEM)
ANY = pl.BlockSpec(memory_space=pl.ANY)
HBM = pl.BlockSpec(memory_space=pltpu.MemorySpace.HBM)
MIB = 1 << 20


def same_chip(one, other):
    place = getattr(one, "coords", None)
    return place is not None and one.id != other.id and place == getattr(other, "coords", None)


def exchange_masks(mesh):
    sizes = mesh.shape["ctx"], mesh.shape["head"]
    devices = mesh.devices.transpose([mesh.axis_names.index(n) for n in ("group", "ctx", "head")])
    core = None
    for axis, bit in ((1, (1, 0)), (2, (0, 1))):
        if sizes[axis - 1] > 1 and same_chip(devices[0, 0, 0], devices[(0, *bit)]):
            core = bit
    masks = []
    for axis, size in enumerate(sizes):
        while size > 1:
            size //= 2
            mask = (size, 0) if axis == 0 else (0, size)
            if mask != core:
                masks.append(mask)
    nearest = [mask for mask in masks if mask[1] == 0][-1:]
    masks = [mask for mask in masks if mask not in nearest] + nearest
    if core is not None:
        masks = [(c ^ core[0], h ^ core[1]) for c, h in masks] + [core]
    return masks


def stack_columns(masks, sizes):
    index_of = {(0, 0): 0}
    for bit, (c, h) in enumerate(masks):
        index_of |= {(i ^ c, j ^ h): at ^ (1 << bit) for (i, j), at in index_of.items()}
    ctx_bits = range(sizes[0].bit_length() - 1)
    head_bits = range(sizes[1].bit_length() - 1)
    return [index_of[1 << b, 0] for b in ctx_bits], [index_of[0, 1 << b] for b in head_bits]


def combine(offset, columns):
    index = 0
    for bit, column in enumerate(columns):
        index = index ^ (((offset >> bit) & 1) * column)
    return index


def swap_halves(values):
    half = ROPE // 2
    lane = lax.broadcasted_iota(jnp.int32, values.shape, 1)
    width = values.shape[1]
    return jnp.where(
        lane % ROPE < half, pltpu.roll(values, width - half, 1), pltpu.roll(values, half, 1)
    )


def rotation_tables(place):
    half = ROPE // 2
    lane = lax.broadcasted_iota(jnp.int32, place.shape, 1)
    frequency = jnp.exp(-math.log(10000.0) * (lane % half).astype(F32) / half)
    angle = place.astype(F32) * frequency
    sine = jnp.sin(angle)
    return jnp.cos(angle), jnp.where(lane % ROPE < half, -sine, sine)


def places_of(token, early, late, block_rows):
    return jnp.where(token < block_rows, early, late) * block_rows + token % block_rows


def pack_kernel(latent_hbm, rope_hbm, piece_ref, rope_ref, sems, *, share):
    tokens = latent_hbm.shape[0]
    fold = LANES // ROPE
    rows = share // fold
    first = pl.multiple_of(lax.axis_index("head") * share, share)
    latent_copy = pltpu.make_async_copy(latent_hbm, piece_ref.at[pl.ds(0, tokens)], sems.at[0])
    rope_copy = pltpu.make_async_copy(rope_hbm.at[pl.ds(first, share)], rope_ref, sems.at[1])
    latent_copy.start()
    rope_copy.start()
    rope_copy.wait()
    mine = rope_ref[...].astype(F32)
    parts = [mine[f * rows : (f + 1) * rows] for f in range(fold)]
    piece_ref[tokens:] = jnp.concatenate(parts, 1).astype(BF16)
    latent_copy.wait()


def absorb_into(query_ref, nope_ref, w_key_ref):
    tokens = nope_ref.shape[0]
    width = w_key_ref.shape[0]
    for head in range(w_key_ref.shape[1] // NOPE):
        columns = slice(head * NOPE, (head + 1) * NOPE)
        absorbed = lax.dot_general(
            nope_ref[:, columns],
            w_key_ref[:, columns],
            (((1,), (1,)), ((), ())),
            preferred_element_type=F32,
        )
        query_ref[head * tokens : (head + 1) * tokens, :width] = absorbed.astype(BF16)


def absorb_kernel(
    cos_ref, sin_ref, nope_ref, rope_ref, top_ref, w_key_hbm, query_ref, bottom_ref, sems
):
    tokens = nope_ref.shape[0]
    part = top_ref.shape[0]
    heads = top_ref.shape[1] // NOPE
    fold = LANES // ROPE
    rest = bottom_ref.shape[0]
    bottom_copy = pltpu.make_async_copy(w_key_hbm.at[pl.ds(part, rest)], bottom_ref, sems.at[0])
    bottom_copy.start()
    absorb_into(query_ref, nope_ref, top_ref)
    lane = lax.broadcasted_iota(jnp.int32, (tokens, LANES), 1)
    for pair in range(heads // fold):
        values = rope_ref[:, pair * LANES : (pair + 1) * LANES].astype(F32)
        rotated = values * cos_ref[...] + swap_halves(values) * sin_ref[...]
        for f in range(fold):
            head = pair * fold + f
            kept = jnp.where(lane // ROPE == f, rotated, 0.0)
            query_ref[head * tokens : (head + 1) * tokens, part:] = kept.astype(BF16)
    bottom_copy.wait()


def absorb_rest_kernel(_, nope_ref, bottom_ref, query_ref):
    absorb_into(query_ref, nope_ref, bottom_ref)


def table_kernel(
    _,
    order_hbm,
    nope_hbm,
    rope_hbm,
    w_key_hbm,
    query_cos_ref,
    query_sin_ref,
    cos_ref,
    sin_ref,
    bias_ref,
    nope_ref,
    rope_ref,
    top_ref,
    order_ref,
    sems,
    *,
    share,
):
    tokens = query_cos_ref.shape[0]
    fold = LANES // ROPE
    rows = share // fold
    block_rows = tokens // 2
    ctx_count, table_rows, _ = cos_ref.shape
    order_copy = pltpu.make_async_copy(order_hbm, order_ref, sems.at[0])
    copies = [
        pltpu.make_async_copy(w_key_hbm.at[pl.ds(0, top_ref.shape[0])], top_ref, sems.at[1]),
        pltpu.make_async_copy(nope_hbm, nope_ref, sems.at[2]),
        pltpu.make_async_copy(rope_hbm, rope_ref, sems.at[3]),
    ]
    order_copy.start()
    for copy in copies:
        copy.start()
    order_copy.wait()
    ctx_here = lax.axis_index("ctx")
    early = order_ref[2 * ctx_here]
    late = order_ref[2 * ctx_here + 1]
    query_token = lax.broadcasted_iota(jnp.int32, (tokens, LANES), 0)
    query_cos_ref[...], query_sin_ref[...] = rotation_tables(
        places_of(query_token, early, late, block_rows)
    )
    row = lax.broadcasted_iota(jnp.int32, (table_rows, LANES), 0)
    lane = lax.broadcasted_iota(jnp.int32, (table_rows, LANES), 1)
    token = (row // rows) * share + (lane // ROPE) * rows + row % rows
    blocks, _, block = bias_ref.shape
    chunks_per_block = block // tokens
    query_token = lax.broadcasted_iota(jnp.int32, (tokens, block), 0)
    query_place = places_of(query_token, early, late, block_rows)
    key_lane = lax.broadcasted_iota(jnp.int32, (tokens, block), 1)

    def one(b, unused):
        key_place = None
        for i in range(chunks_per_block):
            c = b * chunks_per_block + i
            source = ctx_here ^ c
            early = order_ref[2 * source]
            late = order_ref[2 * source + 1]
            cos_ref[c], sin_ref[c] = rotation_tables(places_of(token, early, late, block_rows))
            place = places_of(key_lane % tokens, early, late, block_rows)
            key_place = place if i == 0 else jnp.where(key_lane < i * tokens, key_place, place)
        bias_ref[b] = jnp.where(key_place <= query_place, 0.0, NEGATIVE)
        return unused

    if blocks == 1:
        one(0, 0)
    else:
        lax.fori_loop(0, blocks, one, 0)
    for copy in copies:
        copy.wait()


def attend_kernel(
    stack_ref,
    query_ref,
    rest_ref,
    cos_ref,
    sin_ref,
    bias_ref,
    gain_ref,
    w_value_ref,
    out_hbm,
    key_ref,
    out_ref,
    sems,
    *run_refs,
    ctx_columns,
    head_columns,
    share,
    groups,
    ahead,
):
    tokens = bias_ref.shape[1]
    columns = stack_ref.shape[2]
    latent_width = w_value_ref.shape[0]
    heads = w_value_ref.shape[1] // VALUE_DIM
    ctx_count = cos_ref.shape[0]
    head_count = latent_width // columns
    fold = LANES // ROPE
    rope_rows = share // fold
    starts = [sum(groups[:g]) for g in range(len(groups))]
    head_here = lax.axis_index("head")
    places = [combine(head_here ^ h, head_columns) for h in range(head_count)]
    lane = lax.broadcasted_iota(jnp.int32, (rope_rows, LANES), 1)

    def one_chunk(c, unused):
        first = c * tokens
        if not isinstance(c, int):
            first = pl.multiple_of(first, tokens)
        rows = pl.ds(first, tokens)
        here = combine(c, ctx_columns)
        parts = [stack_ref[p ^ here, :tokens, :].astype(F32) for p in places]
        square = functools.reduce(jnp.add, [x * x for x in parts])
        mean = jnp.sum(square, axis=1, keepdims=True) * (1.0 / latent_width)
        factor = lax.rsqrt(mean + EPSILON)
        for h, x in enumerate(parts):
            gain = gain_ref[:, h * columns : (h + 1) * columns]
            key_ref[rows, h * columns : (h + 1) * columns] = (x * factor * gain).astype(BF16)
        pieces = []
        for h, p in enumerate(places):
            values = stack_ref[p ^ here, tokens:, :].astype(F32)
            table = slice(h * rope_rows, (h + 1) * rope_rows)
            values = values * cos_ref[c, table] + swap_halves(values) * sin_ref[c, table]
            turned = pltpu.roll(values, ROPE, 1)
            pieces.append(jnp.where(lane < ROPE, values, turned))
            pieces.append(jnp.where(lane < ROPE, turned, values))
        key_ref[rows, latent_width:] = jnp.concatenate(pieces, 0).astype(BF16)
        return unused

    if ctx_count <= 8:
        for c in range(ctx_count):
            one_chunk(c, 0)
    else:
        lax.fori_loop(0, ctx_count, one_chunk, 0)

    def scores_of(g, keys):
        first = starts[g] * tokens
        rows = slice(first, first + groups[g] * tokens)
        part = latent_width - rest_ref.shape[1]
        query = jnp.concatenate(
            [query_ref[rows, :part], rest_ref[rows, :], query_ref[rows, part:]], 1
        )
        return lax.dot_general(query, keys, (((1,), (1,)), ((), ())), preferred_element_type=F32)

    def masked(scores, b):
        return scores.reshape(-1, tokens, scores.shape[1]) * SCALE + bias_ref[b][None]

    def out_copy(g):
        where = pl.ds(starts[g] * VALUE_DIM, groups[g] * VALUE_DIM)
        return pltpu.make_async_copy(out_ref.at[:, where], out_hbm.at[:, where], sems.at[g])

    def finish(g, mixed, total):
        mixed = (mixed * (1.0 / total)).astype(BF16)
        for i in range(groups[g]):
            head = starts[g] + i
            where = slice(head * VALUE_DIM, (head + 1) * VALUE_DIM)
            out_ref[:, where] = jnp.dot(
                mixed[i * tokens : (i + 1) * tokens],
                w_value_ref[:, where],
                preferred_element_type=F32,
            ).astype(BF16)
        out_copy(g).start()

    if bias_ref.shape[0] == 1:
        scores = [scores_of(g, key_ref[...]) for g in range(min(ahead, len(groups)))]
        for g in range(len(groups)):
            now = masked(scores[g], 0)
            if g + ahead < len(groups):
                scores.append(scores_of(g + ahead, key_ref[...]))
            exps = jnp.exp2(now - jnp.max(now, axis=2, keepdims=True))
            total = jnp.sum(exps, axis=2, keepdims=True).reshape(-1, 1)
            mixed = jnp.dot(
                exps.reshape(-1, exps.shape[2]).astype(BF16),
                key_ref[:, :latent_width],
                preferred_element_type=F32,
            )
            finish(g, mixed, total)
    else:
        max_ref, total_ref, mixed_ref = run_refs
        block = bias_ref.shape[2]
        for g, group in enumerate(groups):
            height = group * tokens
            rows = slice(0, height)
            max_ref[rows] = jnp.full((height, LANES), NEGATIVE, F32)
            total_ref[rows] = jnp.zeros((height, LANES), F32)
            mixed_ref[rows] = jnp.zeros((height, latent_width), F32)

            def one_block(b, unused):
                keys = key_ref[pl.ds(pl.multiple_of(b * block, block), block), :]
                now = masked(scores_of(g, keys), b)
                old = max_ref[rows, :1].reshape(group, tokens, 1)
                new = jnp.maximum(old, jnp.max(now, axis=2, keepdims=True))
                exps = jnp.where(bias_ref[b][None] < 0.0, 0.0, jnp.exp2(now - new))
                shrink = jnp.exp2(old - new).reshape(height, 1)
                total = jnp.sum(exps, axis=2, keepdims=True).reshape(height, 1)
                max_ref[rows] = jnp.broadcast_to(new.reshape(height, 1), (height, LANES))
                total_ref[rows] = total_ref[rows] * shrink + total
                mixed_ref[rows] = mixed_ref[rows] * shrink + jnp.dot(
                    exps.reshape(height, block).astype(BF16),
                    keys[:, :latent_width],
                    preferred_element_type=F32,
                )
                return unused

            lax.fori_loop(0, bias_ref.shape[0], one_block, 0)
            finish(g, mixed_ref[rows], total_ref[rows, :1])
    for g in range(len(groups)):
        out_copy(g).wait()


def head_groups(heads):
    if heads < 3:
        return [heads]
    return [heads // 3, heads - 2 * (heads // 3), heads // 3]


def make_per_device(sizes, masks):
    ctx_size, head_size = sizes
    ctx_columns, head_columns = stack_columns(masks, sizes)
    everyone = [(c, h) for c in range(ctx_size) for h in range(head_size)]

    def exchange(stack, mask):
        pairs = [
            (c * head_size + h, (c ^ mask[0]) * head_size + (h ^ mask[1])) for c, h in everyone
        ]
        return lax.ppermute(stack, ("ctx", "head"), pairs)

    def per_device(
        query_nope, query_rope, kv_latent, key_rope, latent_gain, w_key, w_value, block_order
    ):
        tokens, columns = kv_latent.shape
        heads = w_key.shape[1] // NOPE
        latent_width = w_key.shape[0]
        query_nope, query_rope, kv_latent, key_rope, w_key, block_order = (
            pltpu.with_memory_space_constraint(x, pltpu.MemorySpace.HBM)
            for x in (query_nope, query_rope, kv_latent, key_rope, w_key, block_order)
        )
        share = tokens // head_size
        rope_rows = share * ROPE // LANES
        groups = head_groups(heads)
        chunks_per_block = min(ctx_size, max(1, 256 // tokens))
        blocks = ctx_size // chunks_per_block

        half_key = jax.ShapeDtypeStruct((latent_width // 2, heads * NOPE), BF16)

        def tables(after):
            query_table = jax.ShapeDtypeStruct((tokens, LANES), F32)
            table = jax.ShapeDtypeStruct((ctx_size, head_size * rope_rows, LANES), F32)
            bias = jax.ShapeDtypeStruct((blocks, tokens, chunks_per_block * tokens), F32)
            nope = jax.ShapeDtypeStruct((tokens, heads * NOPE), BF16)
            rope = jax.ShapeDtypeStruct((tokens, heads * ROPE), BF16)
            return pl.pallas_call(
                functools.partial(table_kernel, share=share),
                out_shape=(query_table, query_table, table, table, bias, nope, rope, half_key),
                in_specs=[ANY] + [HBM] * 4,
                out_specs=(VMEM,) * 8,
                scratch_shapes=[
                    pltpu.SMEM(block_order.shape, jnp.int32),
                    pltpu.SemaphoreType.DMA((4,)),
                ],
                compiler_params=pltpu.CompilerParams(vmem_limit_bytes=8 * MIB),
                name="tables",
            )(after, block_order, query_nope, query_rope, w_key)

        def absorb(*arrays):
            return pl.pallas_call(
                absorb_kernel,
                out_shape=(
                    jax.ShapeDtypeStruct((heads * tokens, latent_width // 2 + LANES), BF16),
                    half_key,
                ),
                in_specs=[VMEM] * 5 + [HBM],
                out_specs=(VMEM, VMEM),
                scratch_shapes=[pltpu.SemaphoreType.DMA((1,))],
                compiler_params=pltpu.CompilerParams(vmem_limit_bytes=8 * MIB),
                name="absorb",
            )(*arrays, w_key)

        def absorb_rest(after, nope, bottom):
            return pl.pallas_call(
                absorb_rest_kernel,
                out_shape=jax.ShapeDtypeStruct((heads * tokens, latent_width // 2), BF16),
                in_specs=[ANY, VMEM, VMEM],
                out_specs=VMEM,
                compiler_params=pltpu.CompilerParams(vmem_limit_bytes=8 * MIB),
                name="absorb_rest",
            )(after, nope, bottom)

        piece = pl.pallas_call(
            functools.partial(pack_kernel, share=share),
            out_shape=jax.ShapeDtypeStruct((tokens + rope_rows, columns), BF16),
            in_specs=[HBM, HBM],
            out_specs=VMEM,
            scratch_shapes=[
                pltpu.VMEM((share, ROPE), BF16),
                pltpu.SemaphoreType.DMA((2,)),
            ],
            compiler_params=pltpu.CompilerParams(vmem_limit_bytes=2 * MIB),
            name="pack",
        )(kv_latent, key_rope)

        stack = piece[None]
        for number, mask in enumerate(masks[:-2]):
            received = exchange(stack, mask)
            if number == len(masks) - 4:
                received, query_cos, query_sin, cosine, sine, bias, nope, rope, top = (
                    lax.optimization_barrier((received, *tables(stack)))
                )
            elif number == len(masks) - 3:
                early = exchange(stack, masks[-2])
                fresh = received
            stack = jnp.concatenate([stack, received], 0)
        received = exchange(fresh, masks[-2])
        _, *arrays = lax.optimization_barrier((fresh, query_cos, query_sin, nope, rope, top))
        received, early, query, bottom = lax.optimization_barrier(
            (received, early, *absorb(*arrays))
        )
        stack = jnp.concatenate([stack, early, received], 0)
        received = exchange(stack, masks[-1])
        received, rest = lax.optimization_barrier((received, absorb_rest(stack, nope, bottom)))
        stack = jnp.concatenate([stack, received], 0)

        keys = ctx_size * tokens
        scratch = [
            pltpu.VMEM((keys, latent_width + LANES), BF16),
            pltpu.VMEM((tokens, heads * VALUE_DIM), BF16),
            pltpu.SemaphoreType.DMA((len(groups),)),
        ]
        if blocks > 1:
            scratch += [
                pltpu.VMEM((max(groups) * tokens, LANES), F32),
                pltpu.VMEM((max(groups) * tokens, LANES), F32),
                pltpu.VMEM((max(groups) * tokens, latent_width), F32),
            ]
        return pl.pallas_call(
            functools.partial(
                attend_kernel,
                ctx_columns=ctx_columns,
                head_columns=head_columns,
                share=share,
                groups=groups,
                ahead=2,
            ),
            out_shape=jax.ShapeDtypeStruct((tokens, heads * VALUE_DIM), BF16),
            in_specs=[VMEM] * 8,
            out_specs=HBM,
            scratch_shapes=scratch,
            compiler_params=pltpu.CompilerParams(vmem_limit_bytes=24 * MIB),
            name="attend",
        )(stack, query, rest, cosine, sine, bias, latent_gain.reshape(1, latent_width), w_value)

    return per_device


def solution(mesh):
    sizes = mesh.shape["ctx"], mesh.shape["head"]
    return jax.shard_map(
        make_per_device(sizes, exchange_masks(mesh)),
        mesh=mesh,
        in_specs=(
            P(("group", "ctx"), "head"),
            P(("group", "ctx"), "head"),
            P(("group", "ctx"), "head"),
            P(("group", "ctx"), None),
            P(),
            P(None, "head"),
            P(None, "head"),
            P("group"),
        ),
        out_specs=P(("group", "ctx"), "head"),
        check_vma=False,
    )
```
